32 devices in a mesh: groups: 2 (over y), slab: 4 (over z), pencil: 2 (over x), comp: 2 (over core).
Axes of the slice: x: 2, y: 2, z: 4, core: 2. Of those that a mesh axis runs over, the one named last changes fastest.
Arguments:
- u_start: float32 [3, 64, 64, 512], P(None, ('groups', 'slab'), 'pencil', 'comp'), parts along dimension 1, may hold values from -6 to 6
- toughness: float32 [64, 64, 512], P(('groups', 'slab'), 'pencil', 'comp'), parts along dimension 0, may hold values from 0.3 to 1.5
- crack_label: int32 [64, 64, 512], P(('groups', 'slab'), 'pencil', 'comp'), parts along dimension 0, may hold values from 0 to 2
- obs_weight: bfloat16 [32, 64, 2, 4096], P('slab', 'pencil', 'comp'), may hold values from -0.75 to 0.75
- sensor_cell: int32 [4096], replicated, may hold values from 0 to 4095
Outputs:
- moved: float32 [3, 64, 64, 512], P(None, ('groups', 'slab'), 'pencil', 'comp'), parts along dimension 1
- damage: float32 [64, 64, 512], P(('groups', 'slab'), 'pencil', 'comp'), parts along dimension 0
- readings: float32 [3, 8192], P(None, 'groups'), parts along dimension 1
The draws below stay inside these ranges and needn't reach their ends.
There are 2 independent parts, one for each index of `groups`. The reference program is written for one: setup_inputs(seed, part) draws one part's arguments, and reference() takes and returns one part's arrays. A program takes and returns all parts, laid end to end along the dimension named above; an argument that names none is the same for every part. Nothing has to cross between parts.
Inputs may be any that keep to these rules, and one draw needn't show every extreme that they name: `sensor_cell`: numbers cell blocks as (64 z + y) * 2 + h. `crack_label`: 0 intact, 1 partly cracked, 2 cracked.
All inputs are finite; a program needn't handle non-finite values.
Results may differ from the reference program's by a relative error of at most 0.003.
Values sent between devices are 32-bit elements; how exact they have to be, the bound alone decides.
A program may use at most 128 MiB of HBM per device.

```python
import math
import jax
import jax.numpy as jnp

CX = 256
SENSORS = 4096
NZ = 32
NY = 64
NX = 512
BLOCKS = 4096
N_COMP = 2


def set_ends(array, rng, least, largest):
    longest = array.shape.index(max(array.shape))
    spots = []
    for shift in (0, 1):
        where = [jax.random.randint(jax.random.fold_in(rng, axis), (), 0, length) for axis, length in enumerate(array.shape)]
        where[longest] = (where[longest] + shift) % array.shape[longest]
        spots.append(tuple(where))
    return array.at[spots[0]].set(least).at[spots[1]].set(largest)


def steps_of(key, extent, cuts, low, largest):
    def one(dim, shards_of):
        heights = jax.random.uniform(jax.random.fold_in(jax.random.fold_in(key, 6), dim), (shards_of,), jnp.float32, low / len(cuts), largest / len(cuts))
        return jnp.repeat(jnp.exp(heights), extent[dim] // shards_of).reshape((-1,) + (1,) * (len(extent) - dim - 1))

    gain = one(*cuts[0])
    for cut in cuts[1:]:
        gain = gain * one(*cut)
    return gain


def normal_values(stream_key, extent, width, limit, cuts=(), held_as=jnp.bfloat16):
    loudness = steps_of(stream_key, extent, cuts, -0.22, 0.18) if cuts else 1.0
    array = jax.random.normal(stream_key, extent, jnp.float32) * width * loudness
    return jnp.minimum(jnp.maximum(array, -limit), limit).astype(held_as)


def setup_inputs(seed: int = 0, part: int = 0) -> dict:
    key_list = jax.random.split(jax.random.key(seed), 6)
    part_splits = jax.random.split(jax.random.fold_in(key_list[5], part), 6)
    u_start = normal_values(part_splits[0], (3, NZ, NY, NX), 1.0, 6.0, ((1, 4), (2, 2), (3, 2)), jnp.float32)
    toughness = jnp.clip(jnp.exp(math.log(1.5) - 1.60943787 * jax.random.uniform(part_splits[1], (NZ, NY, NX), jnp.float32) ** steps_of(part_splits[1], (NZ, NY, NX), ((0, 4), (1, 2), (2, 2)), -0.2, 0.2)), 0.3, 1.5)
    crack_label = set_ends(jax.random.randint(part_splits[2], (NZ, NY, NX), 0, 3), jax.random.fold_in(part_splits[2], 1), 0, 2).astype(jnp.int32)
    obs_weight = normal_values(key_list[3], (NZ, NY, N_COMP, SENSORS), (BLOCKS // 64) ** -0.5, 0.75, ((0, 4), (1, 2), (2, 2)))
    sensor_cell = set_ends(jax.random.randint(key_list[4], (SENSORS,), 0, BLOCKS), jax.random.fold_in(key_list[4], 1), 0, BLOCKS - 1).astype(jnp.int32)
    return dict(u_start=u_start, toughness=toughness, crack_label=crack_label, obs_weight=obs_weight, sensor_cell=sensor_cell)


SHEAR_MODULUS = 1.0
LAME_FIRST = 1.5
RESIDUAL_STIFF = 0.001
TIME_DISP = 0.15
TIME_DAMAGE = 0.08
LENGTH_SCALE = 1.0
DAMAGE_LEVEL = 0.45
POINT_GAIN = 8.0


def central(source, spatial):
    if spatial == 0:
        return 0.5 * (source[..., 2:, 1:-1, 1:-1] - source[..., :-2, 1:-1, 1:-1])
    if spatial == 1:
        return 0.5 * (source[..., 1:-1, 2:, 1:-1] - source[..., 1:-1, :-2, 1:-1])
    return 0.5 * (source[..., 1:-1, 1:-1, 2:] - source[..., 1:-1, 1:-1, :-2])


def shrink(source):
    return source[..., 1:-1, 1:-1, 1:-1]


def laplace(source):
    return (source[2:, 1:-1, 1:-1] + source[:-2, 1:-1, 1:-1] + source[1:-1, 2:, 1:-1]
            + source[1:-1, :-2, 1:-1] + source[1:-1, 1:-1, 2:] + source[1:-1, 1:-1, :-2]
            - 6.0 * source[1:-1, 1:-1, 1:-1])


def entry_key(first, second):
    return (min(first, second), max(first, second))


def rotate(matrix, first, second):
    other = 3 - first - second
    diag_first = matrix[(first, first)]
    diag_second = matrix[(second, second)]
    coupling = matrix[(first, second)]
    angle = 0.5 * jnp.arctan2(2.0 * coupling, diag_second - diag_first)
    cosine = jnp.cos(angle)
    sine = jnp.sin(angle)
    side_first = matrix[entry_key(other, first)]
    side_second = matrix[entry_key(other, second)]
    result = dict(matrix)
    result[(first, first)] = cosine * cosine * diag_first - 2.0 * cosine * sine * coupling + sine * sine * diag_second
    result[(second, second)] = sine * sine * diag_first + 2.0 * cosine * sine * coupling + cosine * cosine * diag_second
    result[(first, second)] = jnp.zeros_like(coupling)
    result[entry_key(other, first)] = cosine * side_first - sine * side_second
    result[entry_key(other, second)] = sine * side_first + cosine * side_second
    return result


def eigenvalues(matrix):
    for sweep_index in range(5):
        for first, second in ((0, 1), (0, 2), (1, 2)):
            matrix = rotate(matrix, first, second)
    return [matrix[(0, 0)], matrix[(1, 1)], matrix[(2, 2)]]


def advance(padded_disp, padded_damage, toughness):
    gradient = [[central(padded_disp[component], direction) for direction in range(3)] for component in range(3)]
    strain = {}
    for first in range(3):
        for second in range(first, 3):
            strain[(first, second)] = 0.5 * (gradient[first][second] + gradient[second][first])
    trace_full = strain[(0, 0)] + strain[(1, 1)] + strain[(2, 2)]
    damage_mid = shrink(padded_damage)
    degrade = (1.0 - damage_mid) ** 2 + RESIDUAL_STIFF
    divergence = []
    for component in range(3):
        total_force = 0.0
        for direction in range(3):
            stress = 2.0 * SHEAR_MODULUS * strain[entry_key(component, direction)]
            if component == direction:
                stress = stress + LAME_FIRST * trace_full
            total_force = total_force + central(degrade * stress, direction)
        divergence.append(total_force)
    moved = shrink(shrink(padded_disp)) + TIME_DISP * jnp.stack(divergence)
    inner = {key_pair: shrink(entry_value) for key_pair, entry_value in strain.items()}
    trace_inner = shrink(trace_full)
    energy = 0.5 * LAME_FIRST * jnp.maximum(trace_inner, 0.0) ** 2
    for eigen_value in eigenvalues(inner):
        energy = energy + SHEAR_MODULUS * jnp.maximum(eigen_value, 0.0) ** 2
    damage_core = shrink(damage_mid)
    damage = damage_core + TIME_DAMAGE * (2.0 * (1.0 - damage_core) * energy
                                          - toughness / LENGTH_SCALE * damage_core
                                          + toughness * LENGTH_SCALE * laplace(damage_mid))
    return moved, damage


def reference(u_start, toughness, crack_label, obs_weight, sensor_cell):
    damage = DAMAGE_LEVEL * crack_label.astype(jnp.float32)
    moved = u_start
    for repeat in range(2):
        padded_disp = jnp.pad(moved, ((0, 0), (2, 2), (2, 2), (2, 2)))
        padded_damage = jnp.pad(damage, 2)
        moved, damage = advance(padded_disp, padded_damage, toughness)
    pooled = jnp.mean(moved.reshape(3, NZ, NY, N_COMP, CX), axis=-1)
    pooled = pooled.reshape(3, NZ * NY * N_COMP).astype(jnp.bfloat16)
    dense = jnp.dot(pooled, obs_weight.reshape(NZ * NY * N_COMP, SENSORS), preferred_element_type=jnp.float32)
    point = pooled.astype(jnp.float32)[:, sensor_cell]
    readings = dense + POINT_GAIN * point
    return moved, damage, readings
```

```python
import itertools

import jax
import jax.numpy as jnp
import numpy as np
from jax import lax
from jax.experimental import pallas as pl
from jax.experimental.pallas import tpu as pltpu
from jax.sharding import PartitionSpec as P

RESIDUAL_STIFF = 0.001
TIME_DISP = 0.15
TIME_DAMAGE = 0.08
DAMAGE_LEVEL = 0.45
POINT_GAIN = 8.0
AXES = ("slab", "pencil", "comp")
MESH = pl.DeviceIdType.MESH
F32 = jnp.float32


def third_angle_poly():
    nodes = 0.5 + 0.5 * np.cos(np.pi * (np.arange(200) + 0.5) / 200)
    fit = np.polynomial.chebyshev.Chebyshev.fit(
        nodes, np.cos(np.arccos(nodes) / 3.0), 8, domain=[0.0, 1.0]
    )
    return [float(c) for c in fit.convert(kind=np.polynomial.Polynomial).coef]


POLY = third_angle_poly()

DIRECTIONS = [
    d for d in itertools.product((-1, 0, 1), repeat=3) if 1 <= sum(map(abs, d)) <= 2
]
ALONG_Z = [d for d in DIRECTIONS if d[0] and not d[1] and not d[2]]
ALONG_Y = [d for d in DIRECTIONS if d[1] and not d[0] and not d[2]]
ALONG_X = [d for d in DIRECTIONS if d[2] and not d[0] and not d[1]]
DIAG_ZY = [d for d in DIRECTIONS if d[0] and d[1]]
DIAG_ZX = [d for d in DIRECTIONS if d[0] and d[2]]
DIAG_YX = [d for d in DIRECTIONS if d[1] and d[2]]
KINDS = (
    [("zu", d) for d in ALONG_Z] + [("zy", d) for d in DIAG_ZY] + [("zx", d) for d in DIAG_ZX]
    + [("zd", d) for d in ALONG_Z] + [("zs", d) for d in ALONG_Z]
    + [(k, d) for k in ("y0", "y1", "y2") for d in ALONG_Y]
    + [(k, d) for k in ("yx0", "yx1") for d in DIAG_YX]
    + [(k, d) for k in ("x0", "x1", "x2") for d in ALONG_X]
)
EDGE = ("zu", "zy", "zx")
REST = ("zd", "zs")


def energy_of(e00, e11, e22, e01, e02, e12):
    trace = e00 + e11 + e22
    mean = trace * (1.0 / 3.0)
    d0, d1, d2 = e00 - mean, e11 - mean, e22 - mean
    p2 = (d0 * d0 + d1 * d1 + d2 * d2) * (1.0 / 6.0) + (
        e01 * e01 + e02 * e02 + e12 * e12
    ) * (1.0 / 3.0)
    inv = lax.rsqrt(jnp.maximum(p2, 1e-36))
    p = p2 * inv
    b0, b1, b2 = d0 * inv, d1 * inv, d2 * inv
    b01, b02, b12 = e01 * inv, e02 * inv, e12 * inv
    half_det = 0.5 * (
        b0 * (b1 * b2 - b12 * b12)
        - b01 * (b01 * b2 - b12 * b02)
        + b02 * (b01 * b12 - b1 * b02)
    )
    r = jnp.minimum(jnp.abs(half_det), 1.0)
    c = jnp.full_like(r, POLY[-1])
    for coefficient in POLY[-2::-1]:
        c = c * r + coefficient
    tc = p * c
    t = jnp.where(half_det < 0.0, -tc, tc)
    s2 = jnp.maximum(1.0 - c * c, 0.0)
    delta = p * (s2 * lax.rsqrt(jnp.maximum(s2, 1e-30))) * float(np.sqrt(3.0))
    f1 = jnp.maximum(mean + 2.0 * t, 0.0)
    f2 = jnp.maximum(mean - t + delta, 0.0)
    f3 = jnp.maximum(mean - t - delta, 0.0)
    ft = jnp.maximum(trace, 0.0)
    return 0.75 * ft * ft + f1 * f1 + f2 * f2 + f3 * f3


def make_kernel(planes, rows, columns, sensors, sizes, first_owner, owners):
    n_slab, n_pencil, n_comp = sizes
    count = n_slab * n_pencil * n_comp
    Z, R, C = planes, rows, columns
    piece = sensors // owners
    half = piece // 2
    rim = 4 * R
    spans = {
        0: {"0": (0, Z)},
        1: {"0": (2, Z - 2), "1": (0, 2), "2": (Z - 2, Z)},
    }
    groups = {0: [range(Z)], 1: [range(2, Z - 2), [0, 1, Z - 2, Z - 1]]}
    near = n_slab <= 4 and n_pencil <= 2 and n_comp <= 2

    def scope(name):
        return jax.named_scope(name)

    def kernel(u_hbm, tough_hbm, crack_hbm, weight_hbm, cell_hbm,
               moved_ref, damage_ref, read_ref,
               U, XR, XS, XC, YR, YP, YZ, YX, YXR, TZ, tough, crack, weight, cell_ref, pooled_t, acc,
               partial, RB, GB,
               in_sem, send_sem, recv_sem, rs_send, rs_recv, ag_send, ag_recv):
        me = [lax.axis_index(a) for a in AXES]
        flat = (me[0] * n_pencil + me[1]) * n_comp + me[2]

        def device(index):
            return {
                "slab": index // (n_pencil * n_comp),
                "pencil": (index // n_comp) % n_pencil,
                "comp": index % n_comp,
            }

        def u_load(k, low, high):
            return pltpu.make_async_copy(
                u_hbm.at[:, low:high], U.at[0, 0:3, low + 2:high + 2, 0:R, 0:C], in_sem.at[k]
            )

        u_loads = [u_load(0, 0, 2), u_load(1, Z - 2, Z), u_load(2, 2, Z - 2)]
        crack_load = pltpu.make_async_copy(crack_hbm, crack, in_sem.at[3])
        tough_load = pltpu.make_async_copy(tough_hbm, tough, in_sem.at[4])
        cell_load = pltpu.make_async_copy(cell_hbm, cell_ref, in_sem.at[5])
        inner = Z * R - rim
        weight_loads = [
            pltpu.make_async_copy(weight_hbm.at[0:rim // 2], weight.at[0, 0:rim // 2], in_sem.at[6]),
            pltpu.make_async_copy(
                weight_hbm.at[Z * R - rim // 2:Z * R], weight.at[0, rim // 2:rim], in_sem.at[7]),
            pltpu.make_async_copy(
                weight_hbm.at[rim // 2:Z * R - rim // 2], weight.at[1, 0:inner], in_sem.at[8]),
        ]
        for load in [*u_loads, crack_load, cell_load, tough_load, *weight_loads]:
            load.start()

        barrier = pltpu.get_barrier_semaphore()

        def inside(d, sign):
            ok = None
            for m, o, n in zip(me, d, sizes):
                if o:
                    here = m + 1 < n if sign * o > 0 else m >= 1
                    ok = here if ok is None else jnp.logical_and(ok, here)
            return ok

        def feasible(d):
            return all(n > 1 for o, n in zip(d, sizes) if o)

        def neighbour(d):
            return {a: m + o for a, m, o in zip(AXES, me, d)}

        met = 0
        if near:
            for d in DIRECTIONS:
                if feasible(d):
                    @pl.when(inside(d, 1))
                    def _():
                        pl.semaphore_signal(
                            barrier, inc=1, device_id=neighbour(d), device_id_type=MESH
                        )

                    met = met + inside(d, 1).astype(jnp.int32)
        else:
            def greet(k, carry):
                pl.semaphore_signal(
                    barrier, inc=1, device_id=device((flat + k) % count), device_id_type=MESH
                )
                return carry

            lax.fori_loop(1, count, greet, 0)
            met = count - 1

        def clear(d, write):
            if feasible(d):
                @pl.when(jnp.logical_not(inside(d, 1)))
                def _():
                    write()
            else:
                write()

        def clear_z(up):
            def write():
                for step in range(2):
                    for z in ((Z + 2, Z + 3) if up else (0, 1)):
                        U[step, :, z, 0:R, 0:C] = jnp.zeros((4, R, C), F32)
                XC[:, up] = jnp.zeros((2, 2, R, 128), F32)
                for step in range(2):
                    for side in range(2):
                        YR[step, side, (Z + 1) * up] = jnp.zeros((8, C), F32)
            return write

        def clear_x(right):
            def write():
                def one(k, carry):
                    XR[k // (4 * Z), right, (k // Z) % 4, k % Z] = jnp.zeros((R, 128), F32)
                    return carry

                lax.fori_loop(0, 8 * Z, one, 0)
                XC[:, :, right] = jnp.zeros((2, 2, R, 128), F32)
                YXR[:, :, right] = jnp.zeros((2, 2, 2, 8, 128), F32)
            return write

        def clear_y(up):
            def write():
                YR[:, up] = jnp.zeros((2, Z + 2, 8, C), F32)
                YXR[:, up] = jnp.zeros((2, 2, 2, 8, 128), F32)
            return write

        for side, sign in ((0, -1), (1, 1)):
            clear((sign, 0, 0), clear_z(side))
            clear((0, sign, 0), clear_y(side))
            clear((0, 0, sign), clear_x(side))

        row8 = lax.broadcasted_iota(jnp.int32, (8, C), 0)
        row8t = lax.broadcasted_iota(jnp.int32, (8, 128), 0)
        lane8 = lax.broadcasted_iota(jnp.int32, (8, 128), 1)
        lane_r = lax.broadcasted_iota(jnp.int32, (R, 128), 1)

        def roll(value, shift, axis):
            shift = shift % value.shape[axis]
            return pltpu.roll(value, shift, axis) if shift else value

        def loop(start, stop, function):
            def one(z, carry):
                function(z)
                return carry

            lax.fori_loop(start, stop, one, 0)

        def message(step, kind, d):
            dz, dy, dx = d
            sz, sy, sx = (dz + 1) // 2, (dy + 1) // 2, (dx + 1) // 2
            lanes = slice(C - 128, C) if dx > 0 else slice(0, 128)
            edge = Z - 1 if dz > 0 else 0
            halo = 0 if dz > 0 else Z + 1
            if kind == "zu":
                pair = (U.at[step, 0:3, edge + 2, 0:R, 0:C], U.at[step, 0:3, halo + 1, 0:R, 0:C])
            elif kind == "zs":
                pair = (
                    U.at[step, 0:3, Z if dz > 0 else 3, 0:R, 0:C],
                    U.at[step, 0:3, 0 if dz > 0 else Z + 3, 0:R, 0:C],
                )
            elif kind == "zd":
                pair = (U.at[step, 3, edge + 2, 0:R, 0:C], U.at[step, 3, halo + 1, 0:R, 0:C])
            elif kind == "zy":
                pair = (YZ.at[step, sy, sz], YR.at[step, 1 - sy, halo])
            elif kind == "zx":
                pair = (XS.at[step, sz, sx], XC.at[step, 1 - sz, 1 - sx])
            elif kind[:2] == "yx":
                part = int(kind[2])
                pair = (YX.at[step, sy, sx, part], YXR.at[step, 1 - sy, 1 - sx, part])
            else:
                low, high = spans[step][kind[1]]
                if kind[0] == "y":
                    pair = (YP.at[step, sy, low:high], YR.at[step, 1 - sy, low + 1:high + 1])
                else:
                    pair = (
                        U.at[step, :, low + 2:high + 2, 0:R, lanes],
                        XR.at[step, 1 - sx, :, low:high],
                    )
            index = KINDS.index((kind, d))
            return pltpu.make_async_remote_copy(
                src_ref=pair[0],
                dst_ref=pair[1],
                send_sem=send_sem.at[step, index],
                recv_sem=recv_sem.at[step, index],
                device_id=neighbour(d),
                device_id_type=MESH,
            )

        def each(step, kinds, sign, action):
            for name in kinds:
                for kind, d in KINDS:
                    if kind == name and feasible(d):
                        @pl.when(inside(d, sign))
                        def _():
                            action(message(step, kind, d))

        def send(step, *kinds):
            each(step, kinds, 1, lambda copy: copy.start())

        def receive(step, *kinds):
            each(step, kinds, -1, lambda copy: copy.wait_recv())

        def pack_plane(step, z, save):
            low = [U[step, f, z + 2, 0:8, 0:C] for f in range(4)]
            high = [U[step, f, z + 2, R - 8:R, 0:C] for f in range(4)]
            for side, tiles, shifts in (
                (0, low, (0, 2, 4, 6)), (1, high, (2, 4, 6, 7))
            ):
                rolled = [roll(t, s, 0) for t, s in zip(tiles, shifts)]
                save(side, jnp.where(
                    row8 < 2, rolled[0],
                    jnp.where(row8 < 4, rolled[1], jnp.where(row8 < 6, rolled[2], rolled[3])),
                ))

        def pack_y(step, part):
            for z in groups[step][part]:
                def save(side, value):
                    YP[step, side, z] = value

                pack_plane(step, z, save)
            for side in range(2):
                for sx in range(2):
                    tile = jnp.zeros((8, 128), F32)
                    for z in groups[step][part]:
                        value = YP[step, side, z, :, (C - 128) * sx:(C - 128) * sx + 128]
                        tile = jnp.where(lane8 == z, roll(value, z + sx, 1), tile)
                    YX[step, side, sx, part] = tile

        def pack_corners(step):
            for sz, z in ((0, 0), (1, Z - 1)):
                for sx in range(2):
                    tiles = [
                        roll(U[step, f, z + 2, 0:R, (C - 128) * sx:(C - 128) * sx + 128], f + sx, 1)
                        for f in range(3)
                    ]
                    XS[step, sz, sx] = jnp.where(
                        lane_r == 0, tiles[0], jnp.where(lane_r == 1, tiles[1], tiles[2])
                    )

                def save(side, value):
                    YZ[step, side, sz] = value

                pack_plane(step, z, save)

        def merged(low, high, f, row):
            up, down = ((8 - 2 * f) % 8, 6 - 2 * f) if f < 3 else (2, 1)
            return jnp.where(row < 4, roll(high, up, 0), roll(low, down, 0))

        def unpack_x(step, z):
            for f in range(4):
                U[step, f, z + 2, 0:R, C:C + 128] = jnp.where(
                    lane_r < 64, XR[step, 1, f, z], XR[step, 0, f, z]
                )

        def unpack_zx(step):
            for sz, z in ((0, -1), (1, Z)):
                for f in range(3):
                    U[step, f, z + 2, 0:R, C:C + 128] = jnp.where(
                        lane_r < 64, roll(XC[step, sz, 1], -f, 1), roll(XC[step, sz, 0], 127 - f, 1)
                    )

        def unpack_y(step, z, fields):
            low, high = YR[step, 0, z + 1], YR[step, 1, z + 1]
            for f in range(fields):
                U[step, f, z + 2, R:R + 8, 0:C] = merged(low, high, f, row8)

        def unpack_yx(step, part):
            for z in groups[step][part]:
                left, right = [
                    [roll(YXR[step, sy, sx, part], 127 * (1 - sx) - z, 1) for sy in range(2)]
                    for sx in range(2)
                ]
                for f in range(3):
                    U[step, f, z + 2, R:R + 8, C:C + 128] = jnp.where(
                        lane8 < 64, merged(*right, f, row8t), merged(*left, f, row8t)
                    )

        def ends(step, z):
            now = [U[step, i, z + 2] for i in range(3)]
            gz = [
                U[step, i, z + 3, 0:R, 0:C] - U[step, i, z + 1, 0:R, 0:C] for i in range(3)
            ]

            def along(value, axis):
                return (roll(value, -1, axis) - roll(value, 1, axis))[0:R, 0:C]

            gy0, gy1 = along(now[0], 0), along(now[1], 0)
            gx0, gx2 = along(now[0], 1), along(now[2], 1)
            keep = 1.0 - U[step, 3, z + 2, 0:R, 0:C]
            g = (0.5 * TIME_DISP) * (keep * keep + RESIDUAL_STIFF)
            TZ[z + 1, 0] = g * (gz[0] + 0.75 * (gz[0] + gy1 + gx2))
            TZ[z + 1, 1] = g * (0.5 * (gz[1] + gy0))
            TZ[z + 1, 2] = g * (0.5 * (gz[2] + gx0))

        def store(step, f, z, value):
            if step == 0:
                U[1, f, z + 2, 0:R, 0:C] = value
            elif f < 3:
                moved_ref[f, z] = value
            else:
                damage_ref[z] = value

        def load(step, f, z):
            return U[1, f, z + 2, 0:R, 0:C] if step == 0 else moved_ref[f, z]

        def core(value):
            return value[0:R, 0:C]

        def hurt(step, z, gz0, gy1, gx2, s01, s02, s12):
            energy = energy_of(0.5 * gz0, 0.5 * gy1, 0.5 * gx2, 0.5 * s01, 0.5 * s02, 0.5 * s12)
            dy = U[step, 3, z + 2, :, 0:C]
            dx = U[step, 3, z + 2, 0:R]
            dc = U[step, 3, z + 2, 0:R, 0:C]
            lap = (
                U[step, 3, z + 3, 0:R, 0:C] + U[step, 3, z + 1, 0:R, 0:C]
                + (roll(dy, -1, 0) + roll(dy, 1, 0))[0:R]
                + (roll(dx, -1, 1) + roll(dx, 1, 1))[:, 0:C]
                - 6.0 * dc
            )
            store(step, 3, z, dc + TIME_DAMAGE * (
                2.0 * (1.0 - dc) * energy + tough[z] * (lap - dc)
            ))

        def damage(step, z):
            gz = [U[step, i, z + 3, 0:R, 0:C] - U[step, i, z + 1, 0:R, 0:C] for i in range(3)]
            in_rows = [U[step, i, z + 2, :, 0:C] for i in range(3)]
            in_lanes = [U[step, i, z + 2, 0:R, :] for i in range(3)]
            gy = [(roll(v, -1, 0) - roll(v, 1, 0))[0:R] for v in in_rows]
            gx = [(roll(v, -1, 1) - roll(v, 1, 1))[:, 0:C] for v in in_lanes]
            hurt(
                step, z, gz[0], gy[1], gx[2], 0.5 * (gz[1] + gy[0]), 0.5 * (gz[2] + gx[0]),
                0.5 * (gy[2] + gx[1]),
            )

        def force(step, z, with_damage):
            now = [U[step, i, z + 2] for i in range(3)]
            gz = [U[step, i, z + 3] - U[step, i, z + 1] for i in range(3)]
            gy = [roll(v, -1, 0) - roll(v, 1, 0) for v in now]
            gx = [roll(v, -1, 1) - roll(v, 1, 1) for v in now]
            keep = 1.0 - U[step, 3, z + 2]
            g = (0.5 * TIME_DISP) * (keep * keep + RESIDUAL_STIFF)
            lam = 0.75 * (gz[0] + gy[1] + gx[2])
            s01 = 0.5 * (gz[1] + gy[0])
            s02 = 0.5 * (gz[2] + gx[0])
            s12 = 0.5 * (gy[2] + gx[1])
            in_y = [g * s01, g * (gy[1] + lam), g * s12]
            in_x = [(g * s02)[0:R], in_y[2][0:R], (g * (gx[2] + lam))[0:R]]
            TZ[z + 1, 0] = core(g * (gz[0] + lam))
            TZ[z + 1, 1] = core(in_y[0])
            TZ[z + 1, 2] = in_x[0][:, 0:C]
            for i in range(3):
                ty = in_y[i][:, 0:C]
                change = (roll(ty, -1, 0) - roll(ty, 1, 0))[0:R] + (
                    roll(in_x[i], -1, 1) - roll(in_x[i], 1, 1)
                )[:, 0:C]
                store(step, i, z, core(now[i]) + change)
            if with_damage:
                hurt(step, z, core(gz[0]), core(gy[1]), core(gx[2]), core(s01), core(s02), core(s12))

        def finish(step, z):
            for i in range(3):
                store(step, i, z, load(step, i, z) + (TZ[z + 2, i] - TZ[z, i]))

        def finish_pool(z, row):
            means = []
            for i in range(3):
                value = moved_ref[i, z] + (TZ[z + 2, i] - TZ[z, i])
                moved_ref[i, z] = value
                folded = value[:, 0:128]
                for cut in range(128, C, 128):
                    folded = folded + value[:, cut:cut + 128]
                means.append(jnp.sum(folded, axis=1, keepdims=True) * (1.0 / C))
            pooled_t[row:row + R, :] = jnp.where(
                lane_r == 0, means[0], jnp.where(lane_r == 1, means[1], means[2])
            )

        def pooled(rows_here):
            value = pooled_t[0:rows_here, :].T[0:8].astype(jnp.bfloat16)
            return jnp.concatenate([value, value], axis=1)

        crack_load.wait()

        def label(z, carry):
            U[0, 3, z + 2, 0:R, 0:C] = DAMAGE_LEVEL * crack[z].astype(F32)
            return carry

        lax.fori_loop(0, Z, label, 0)
        u_loads[0].wait()
        u_loads[1].wait()
        pack_corners(0)
        with scope("barrier"):
            pl.semaphore_wait(barrier, met)
        send(0, "zu", "zx", "zy", "zd", "zs")
        u_loads[2].wait()
        with scope("pack"):
            pack_y(0, 0)
            send(0, "y0", "yx0", "x0")
        cell_load.wait()
        base = me[0] * Z * (R * n_pencil) + me[1] * R
        row_id = lax.broadcasted_iota(jnp.int32, (R, 512), 0) * n_comp

        def choose(part, z, row):
            start = (base + z * (R * n_pencil)) * n_comp + me[2]
            for s in range(0, sensors, 512):
                hit = row_id == cell_ref[:, s:s + 512] - start
                weight[part, row:row + R, s:s + 512] = jnp.where(hit, POINT_GAIN, 0.0).astype(
                    jnp.bfloat16
                )

        with scope("choose"):
            for k, z in enumerate((0, 1, Z - 2, Z - 1)):
                choose(0, z, rim + k * R)
            for z in range(2, Z - 2):
                choose(1, z, inner + (z - 2) * R)
            tough_load.wait()
        with scope("waitx"):
            receive(0, "x0")
        with scope("unpx"):
            loop(0, Z, lambda z: unpack_x(0, z))
        with scope("waity"):
            receive(0, "y0", "yx0")
        with scope("unpy"):
            loop(0, Z, lambda z: unpack_y(0, z, 4))
            unpack_yx(0, 0)
        with scope("body"):
            loop(1, Z - 1, lambda z: force(0, z, True))
            loop(2, Z - 2, lambda z: finish(0, z))
        with scope("pack1"):
            pack_y(1, 0)
            send(1, "y0", "yx0", "x0")
        with scope("waitza"):
            receive(0, *EDGE)
        with scope("edge"):
            unpack_zx(0)
            for z in (-1, Z):
                unpack_y(0, z, 3)
            loop(0, 2, lambda k: force(0, k * (Z - 1), False))
            loop(0, 2, lambda k: finish(0, 1 + k * (Z - 3)))
        send(1, "zs")
        with scope("waitzb"):
            receive(0, *REST)
        with scope("ends"):
            loop(0, 2, lambda k: ends(0, k * (Z + 1) - 1))
            loop(0, 2, lambda k: finish(0, k * (Z - 1)))
        pack_corners(1)
        send(1, "zu", "zx", "zy")
        with scope("damage"):
            loop(0, 2, lambda k: damage(0, k * (Z - 1)))
        send(1, "zd")
        with scope("pack2"):
            pack_y(1, 1)
            send(1, "y1", "y2", "yx1", "x1", "x2")

        with scope("waitx"):
            receive(1, "x0")
            loop(2, Z - 2, lambda z: unpack_x(1, z))
        with scope("waity"):
            receive(1, "y0", "yx0")
            loop(2, Z - 2, lambda z: unpack_y(1, z, 4))
            unpack_yx(1, 0)
        with scope("body"):
            loop(3, Z - 3, lambda z: force(1, z, False))
        with scope("waitxy"):
            receive(1, "x1", "x2", "y1", "y2", "yx1")
        with scope("unpxy"):
            for z in (0, 1, Z - 2, Z - 1):
                unpack_x(1, z)
                unpack_y(1, z, 4)
            unpack_yx(1, 1)
        with scope("body2"):
            loop(0, 2, lambda k: force(1, 1 + k * (Z - 3), False))
            loop(0, 2, lambda k: force(1, 2 + k * (Z - 5), False))
        with scope("pooli"):
            for z in range(2, Z - 2):
                finish_pool(z, (z - 2) * R)
        with scope("doti"):
            for load in weight_loads:
                load.wait()
            lhs = pooled(inner)
            for cut in range(0, sensors, 256):
                acc[:, cut:cut + 256] = jnp.dot(
                    lhs, weight[1, 0:2 * inner, cut:cut + 256], preferred_element_type=F32
                )
        with scope("waitz"):
            receive(1, *REST, *EDGE)
        with scope("edge"):
            unpack_zx(1)
            for z in (-1, Z):
                unpack_y(1, z, 3)
            loop(0, 2, lambda k: force(1, k * (Z - 1), False))
            loop(0, 2, lambda k: ends(1, k * (Z + 1) - 1))
        with scope("poole"):
            for k, z in enumerate((0, 1, Z - 2, Z - 1)):
                finish_pool(z, k * R)

        def spread(stop, function):
            if stop <= 16:
                for k in range(stop):
                    function(k)
            else:
                loop(0, stop, function)

        def scatter(q):
            return pltpu.make_async_remote_copy(
                src_ref=partial.at[q], dst_ref=RB.at[flat],
                send_sem=rs_send.at[q], recv_sem=rs_recv.at[flat],
                device_id=device(first_owner + q), device_id_type=MESH,
            )

        def scatter_from(k):
            return pltpu.make_async_remote_copy(
                src_ref=partial.at[0], dst_ref=RB.at[k],
                send_sem=rs_send.at[0], recv_sem=rs_recv.at[k],
                device_id=device(k), device_id_type=MESH,
            )

        def gather(q, k):
            return pltpu.make_async_remote_copy(
                src_ref=GB.at[q], dst_ref=GB.at[q],
                send_sem=ag_send.at[k], recv_sem=ag_recv.at[q],
                device_id=device(k), device_id_type=MESH,
            )

        def unless(same, function):
            @pl.when(jnp.logical_not(same))
            def _():
                function()

        mine = flat - first_owner
        owning = jnp.logical_and(mine >= 0, mine < owners)
        with scope("dot"):
            lhs = pooled(rim)
            for q in range(owners):
                for h in range(2):
                    cut = q * piece + h * half
                    value = acc[:, cut:cut + half] + jnp.dot(
                        lhs, weight[0, 0:2 * rim, cut:cut + half], preferred_element_type=F32
                    )
                    partial[q, 4 * h:4 * h + 4] = value[0:4]
                unless(mine == q, lambda: scatter(q).start())

        with scope("damage"):
            loop(0, Z, lambda z: damage(1, z))

        @pl.when(owning)
        def _():
            with scope("waitrs"):
                spread(count, lambda k: unless(flat == k, lambda: scatter_from(k).wait_recv()))
            RB[flat] = partial[mine]
            if count <= 16:
                total = RB[0]
                for k in range(1, count):
                    total = total + RB[k]
            else:
                total = lax.fori_loop(1, count, lambda k, t: t + RB[k], RB[0])
            GB[mine] = total
            spread(count, lambda k: unless(flat == k, lambda: gather(mine, k).start()))

        with scope("waitag"):
            for q in range(owners):
                unless(mine == q, lambda: gather(q, 0).wait_recv())
        for q in range(owners):
            read_ref[:, q * piece:q * piece + half] = GB[q, 0:3]
            read_ref[:, q * piece + half:(q + 1) * piece] = GB[q, 4:7]
        with scope("sends"):
            for step in range(2):
                names = ["zu", "zx", "zy", "zd", "zs", "y0", "yx0", "x0"]
                if step:
                    names += ["y1", "y2", "yx1", "x1", "x2"]
                each(step, names, 1, lambda copy: copy.wait_send())
            for q in range(owners):
                unless(mine == q, lambda: scatter(q).wait_send())

            @pl.when(owning)
            def _():
                spread(count, lambda k: unless(flat == k, lambda: gather(mine, k).wait_send()))

    return kernel


def emit(moved_ref, damage_ref, read_ref, moved_hbm, damage_hbm, read_hbm, sem):
    copies = [
        pltpu.make_async_copy(moved_ref, moved_hbm, sem.at[0]),
        pltpu.make_async_copy(damage_ref, damage_hbm, sem.at[1]),
        pltpu.make_async_copy(read_ref, read_hbm, sem.at[2]),
    ]
    for copy in copies:
        copy.start()
    for copy in copies:
        copy.wait()


def solution(mesh):
    sizes = tuple(mesh.shape[a] for a in AXES)
    n_slab, plane_devices = sizes[0], sizes[1] * sizes[2]
    count = n_slab * plane_devices

    def local(u_start, toughness, crack_label, obs_weight, sensor_cell):
        Z, R, C = toughness.shape
        S = sensor_cell.shape[0]
        first_owner = max(n_slab // 2 - 1, 0) * plane_devices
        owners = min(2, n_slab) * plane_devices
        while S % (owners * 256):
            owners -= 1
        piece = S // owners
        rim, inner = 4 * R, (Z - 4) * R
        any_spec = pl.BlockSpec(memory_space=pltpu.HBM)
        vmem_spec = pl.BlockSpec(memory_space=pltpu.VMEM)
        dma = pltpu.SemaphoreType.DMA
        shapes = (
            jax.ShapeDtypeStruct((3, Z, R, C), F32),
            jax.ShapeDtypeStruct((Z, R, C), F32),
            jax.ShapeDtypeStruct((3, S), F32),
        )
        outs = pl.pallas_call(
            make_kernel(Z, R, C, S, sizes, first_owner, owners),
            out_shape=shapes,
            in_specs=[any_spec] * 5,
            out_specs=[vmem_spec] * 3,
            scratch_shapes=[
                pltpu.VMEM((2, 4, Z + 4, R + 8, C + 128), F32),
                pltpu.VMEM((2, 2, 4, Z, R, 128), F32),
                pltpu.VMEM((2, 2, 2, R, 128), F32),
                pltpu.VMEM((2, 2, 2, R, 128), F32),
                pltpu.VMEM((2, 2, Z + 2, 8, C), F32),
                pltpu.VMEM((2, 2, Z, 8, C), F32),
                pltpu.VMEM((2, 2, 2, 8, C), F32),
                pltpu.VMEM((2, 2, 2, 2, 8, 128), F32),
                pltpu.VMEM((2, 2, 2, 2, 8, 128), F32),
                pltpu.VMEM((Z + 2, 3, R, C), F32),
                pltpu.VMEM((Z, R, C), F32),
                pltpu.VMEM((Z, R, C), jnp.int32),
                pltpu.VMEM((2, 2 * max(rim, inner), S), jnp.bfloat16),
                pltpu.VMEM((1, S), jnp.int32),
                pltpu.VMEM((max(rim, inner), 128), F32),
                pltpu.VMEM((8, S), F32),
                pltpu.VMEM((owners, 8, piece // 2), F32),
                pltpu.VMEM((count, 8, piece // 2), F32),
                pltpu.VMEM((owners, 8, piece // 2), F32),
                dma((9,)),
                dma((2, len(KINDS))),
                dma((2, len(KINDS))),
                dma((owners,)),
                dma((count,)),
                dma((count,)),
                dma((owners,)),
            ],
            compiler_params=pltpu.CompilerParams(
                collective_id=0, has_side_effects=True, vmem_limit_bytes=40 * 1024 * 1024
            ),
            name="fracture",
        )(
            *[
                pltpu.with_memory_space_constraint(x, pltpu.HBM)
                for x in (
                    u_start, toughness, crack_label, obs_weight.reshape(Z * R, S),
                    sensor_cell.reshape(1, S),
                )
            ],
        )
        return pl.pallas_call(
            emit,
            out_shape=shapes,
            in_specs=[vmem_spec] * 3,
            out_specs=[any_spec] * 3,
            scratch_shapes=[dma((3,))],
            name="emit",
        )(*[pltpu.with_memory_space_constraint(x, pltpu.VMEM) for x in outs])

    return jax.shard_map(
        local,
        mesh=mesh,
        in_specs=(
            P(None, ("groups", "slab"), "pencil", "comp"),
            P(("groups", "slab"), "pencil", "comp"),
            P(("groups", "slab"), "pencil", "comp"),
            P("slab", "pencil", "comp", None),
            P(),
        ),
        out_specs=(
            P(None, ("groups", "slab"), "pencil", "comp"),
            P(("groups", "slab"), "pencil", "comp"),
            P(None, "groups"),
        ),
        check_vma=False,
    )
```

```python
import itertools

import jax
import jax.numpy as jnp
import numpy as np
from jax import lax
from jax.experimental import pallas as pl
from jax.experimental.pallas import tpu as pltpu
from jax.sharding import PartitionSpec as P

RESIDUAL_STIFF = 0.001
TIME_DISP = 0.15
TIME_DAMAGE = 0.08
DAMAGE_LEVEL = 0.45
POINT_GAIN = 8.0
AXES = ("slab", "pencil", "comp")
MESH = pl.DeviceIdType.MESH
F32 = jnp.float32


def third_angle_poly():
    nodes = 0.5 + 0.5 * np.cos(np.pi * (np.arange(200) + 0.5) / 200)
    fit = np.polynomial.chebyshev.Chebyshev.fit(
        nodes, np.cos(np.arccos(nodes) / 3.0), 8, domain=[0.0, 1.0]
    )
    return [float(c) for c in fit.convert(kind=np.polynomial.Polynomial).coef]


POLY = third_angle_poly()

DIRECTIONS = [
    d for d in itertools.product((-1, 0, 1), repeat=3) if 1 <= sum(map(abs, d)) <= 2
]
ALONG_Z = [d for d in DIRECTIONS if d[0] and not d[1] and not d[2]]
ALONG_Y = [d for d in DIRECTIONS if d[1] and not d[0] and not d[2]]
ALONG_X = [d for d in DIRECTIONS if d[2] and not d[0] and not d[1]]
DIAG_ZY = [d for d in DIRECTIONS if d[0] and d[1]]
DIAG_ZX = [d for d in DIRECTIONS if d[0] and d[2]]
DIAG_YX = [d for d in DIRECTIONS if d[1] and d[2]]
KINDS = (
    [("zu", d) for d in ALONG_Z] + [("zy", d) for d in DIAG_ZY] + [("zx", d) for d in DIAG_ZX]
    + [("zd", d) for d in ALONG_Z] + [("zs", d) for d in ALONG_Z]
    + [(k, d) for k in ("y0", "y1", "y2") for d in ALONG_Y]
    + [(k, d) for k in ("yx0", "yx1") for d in DIAG_YX]
    + [(k, d) for k in ("x0", "x1", "x2") for d in ALONG_X]
)
EDGE = ("zu", "zy", "zx")
REST = ("zd", "zs")


def energy_of(g0, g1, g2, a01, a02, a12):
    trace = g0 + g1 + g2
    mean = trace * (1.0 / 3.0)
    d0, d1, d2 = g0 - mean, g1 - mean, g2 - mean
    q01, q02, q12 = a01 * a01, a02 * a02, a12 * a12
    d01 = d0 * d1
    p2 = (d0 * d0 + d1 * d1 + d01) * (1.0 / 3.0) + (q01 + q02 + q12) * (1.0 / 12.0)
    inv = lax.rsqrt(jnp.maximum(p2, 1e-36))
    p = p2 * inv
    det = d01 * d2 + 0.25 * (a01 * a02 * a12 - d0 * q12 - d1 * q02 - d2 * q01)
    half_det = ((det * inv) * inv) * (0.5 * inv)
    r = jnp.minimum(jnp.abs(half_det), 1.0)
    c = jnp.full_like(r, POLY[-1])
    for coefficient in POLY[-2::-1]:
        c = c * r + coefficient
    tc = p * c
    t = jnp.where(half_det < 0.0, -tc, tc)
    s2 = jnp.maximum(1.0 - c * c, 0.0)
    delta = p * (s2 * lax.rsqrt(jnp.maximum(s2, 1e-30))) * float(np.sqrt(3.0))
    f1 = jnp.maximum(mean + 2.0 * t, 0.0)
    f2 = jnp.maximum(mean - t + delta, 0.0)
    f3 = jnp.maximum(mean - t - delta, 0.0)
    ft = jnp.maximum(trace, 0.0)
    return 0.75 * ft * ft + f1 * f1 + f2 * f2 + f3 * f3


def message_tiles(kind, step, Z, R, L):
    if kind in ("zu", "zs"):
        return 3 * L * R // 8
    if kind == "zd":
        return L * R // 8
    if kind == "zx":
        return R // 8
    if kind == "zy":
        return L
    if kind[:2] == "yx":
        return 1
    planes = 2 if kind[1] != "0" else Z - 4 if step else Z
    return planes * L if kind[0] == "y" else planes * 4 * R // 8


SENT = [
    ("zu", "zx", "zy", "zd", "zs", "y0", "yx0", "x0"),
    ("zu", "zx", "zy", "zd", "zs", "y0", "yx0", "x0", "y1", "y2", "yx1", "x1", "x2"),
]


def group_tiles(step, kinds, met, Z, R, L):
    total = 0
    for kind in kinds:
        number = message_tiles(kind, step, Z, R, L)
        axes = [a for a, name in enumerate("zyx") if name in kind[:2]]
        for a in axes if kind[:2] in ("zx", "zy", "yx") else axes[:1]:
            number *= met[a]
        total += number
    return total


def make_kernel(planes, rows, columns, sensors, sizes, first_slab, owners):
    n_slab, n_pencil, n_comp = sizes
    count = n_slab * n_pencil * n_comp
    Z, R, C = planes, rows, columns
    piece = sensors // owners
    strips = piece // 128
    L = C // 128
    TOP = 16
    END = TOP + R
    body_rows = slice(TOP, END)
    rim = 4 * R
    spans = {
        0: {"0": (0, Z)},
        1: {"0": (2, Z - 2), "1": (0, 2), "2": (Z - 2, Z)},
    }
    groups = {0: [range(Z)], 1: [range(2, Z - 2), [0, 1, Z - 2, Z - 1]]}
    near = n_slab <= 4 and n_pencil <= 2 and n_comp <= 2

    def scope(name):
        return jax.named_scope(name)

    def kernel(u_hbm, tough_hbm, crack_hbm, weight_hbm, cell_hbm,
               moved_ref, damage_ref, read_ref,
               U, XR, XS, XC, YR, YP, YZ, YX, YXR, TZ, TY, W, tough, crack, weight, cell_ref, pooled_t, acc,
               partial, RB, GB,
               in_sem, send_sem, recv_sem):
        me = [lax.axis_index(a) for a in AXES]
        flat = (me[0] * n_pencil + me[1]) * n_comp + me[2]

        def device(index):
            return {
                "slab": index // (n_pencil * n_comp),
                "pencil": (index // n_comp) % n_pencil,
                "comp": index % n_comp,
            }

        def u_load(k, low, high):
            return [
                pltpu.make_async_copy(
                    u_hbm.at[:, low:high, :, 128 * l:128 * l + 128],
                    U.at[0, 0:3, low + 2:high + 2, l, body_rows, :],
                    in_sem.at[4 if k == 2 else 0],
                )
                for l in range(L)
            ]

        edge_loads = u_load(0, 0, 2) + u_load(1, Z - 2, Z)
        inner_loads = u_load(2, 2, Z - 2)
        crack_load = pltpu.make_async_copy(crack_hbm, crack, in_sem.at[1])
        tough_load = pltpu.make_async_copy(tough_hbm, tough, in_sem.at[2])
        cell_load = pltpu.make_async_copy(cell_hbm, cell_ref, in_sem.at[3])
        inner = Z * R - rim
        weight_loads = [
            pltpu.make_async_copy(weight_hbm.at[0:rim // 2], weight.at[0, 0:rim // 2], in_sem.at[5]),
            pltpu.make_async_copy(
                weight_hbm.at[Z * R - rim // 2:Z * R], weight.at[0, rim // 2:rim], in_sem.at[5]),
            pltpu.make_async_copy(
                weight_hbm.at[rim // 2:Z * R - rim // 2], weight.at[1, 0:inner], in_sem.at[5]),
        ]
        for item in [*edge_loads, crack_load, *inner_loads, cell_load]:
            item.start()

        barrier = pltpu.get_barrier_semaphore()

        def inside(d, sign):
            ok = None
            for m, o, n in zip(me, d, sizes):
                if o:
                    here = m + 1 < n if sign * o > 0 else m >= 1
                    ok = here if ok is None else jnp.logical_and(ok, here)
            return ok

        def feasible(d):
            return all(n > 1 for o, n in zip(d, sizes) if o)

        def neighbour(d):
            return {a: m + o for a, m, o in zip(AXES, me, d)}

        met = 0
        if near:
            for d in DIRECTIONS:
                if feasible(d):
                    @pl.when(inside(d, 1))
                    def _():
                        pl.semaphore_signal(
                            barrier, inc=1, device_id=neighbour(d), device_id_type=MESH
                        )

                    met = met + inside(d, 1).astype(jnp.int32)
        else:
            def greet(k, carry):
                pl.semaphore_signal(
                    barrier, inc=1, device_id=device((flat + k) % count), device_id_type=MESH
                )
                return carry

            lax.fori_loop(1, count, greet, 0)
            met = count - 1

        def clear(d, write):
            if feasible(d):
                @pl.when(jnp.logical_not(inside(d, 1)))
                def _():
                    write()
            else:
                write()

        def clear_z(up):
            def write():
                for step in range(2):
                    for z in ((Z + 2, Z + 3) if up else (0, 1)):
                        U[step, :, z, 0:L, body_rows] = jnp.zeros((4, L, R, 128), F32)
                XC[:, up] = jnp.zeros((2, 2, R, 128), F32)
                for step in range(2):
                    for side in range(2):
                        YR[step, side, (Z + 1) * up] = jnp.zeros((8, C), F32)
            return write

        def clear_x(right):
            def write():
                def one(k, carry):
                    XR[k // (4 * Z), right, (k // Z) % 4, k % Z] = jnp.zeros((R, 128), F32)
                    return carry

                lax.fori_loop(0, 8 * Z, one, 0)
                XC[:, :, right] = jnp.zeros((2, 2, R, 128), F32)
                YXR[:, :, right] = jnp.zeros((2, 2, 2, 8, 128), F32)
            return write

        def clear_y(up):
            def write():
                YR[:, up] = jnp.zeros((2, Z + 2, 8, C), F32)
                YXR[:, up] = jnp.zeros((2, 2, 2, 8, 128), F32)
            return write

        row8t = lax.broadcasted_iota(jnp.int32, (8, 128), 0)
        lane8 = lax.broadcasted_iota(jnp.int32, (8, 128), 1)
        lane_r = lax.broadcasted_iota(jnp.int32, (R, 128), 1)

        def roll(value, shift, axis):
            shift = shift % value.shape[axis]
            return pltpu.roll(value, shift, axis) if shift else value

        def loop(start, stop, function):
            def one(z, carry):
                function(z)
                return carry

            lax.fori_loop(start, stop, one, 0)

        def slot(step, kind):
            if step == 0:
                return 0 if kind in EDGE else 1 if kind in REST else 2 if kind[0] == "x" else 3
            if kind[0] == "z":
                return 4
            return 7 if kind[-1] != "0" else 5 if kind[0] == "x" else 6

        def message(step, kind, d):
            dz, dy, dx = d
            sz, sy, sx = (dz + 1) // 2, (dy + 1) // 2, (dx + 1) // 2
            tile = L - 1 if dx > 0 else 0
            edge = Z - 1 if dz > 0 else 0
            halo = 0 if dz > 0 else Z + 1
            if kind == "zu":
                pair = (
                    U.at[step, 0:3, edge + 2, 0:L, body_rows], U.at[step, 0:3, halo + 1, 0:L, body_rows]
                )
            elif kind == "zs":
                pair = (
                    U.at[step, 0:3, Z if dz > 0 else 3, 0:L, body_rows],
                    U.at[step, 0:3, 0 if dz > 0 else Z + 3, 0:L, body_rows],
                )
            elif kind == "zd":
                pair = (U.at[step, 3, edge + 2, 0:L, body_rows], U.at[step, 3, halo + 1, 0:L, body_rows])
            elif kind == "zy":
                pair = (YZ.at[step, sy, sz], YR.at[step, 1 - sy, halo])
            elif kind == "zx":
                pair = (XS.at[step, sz, sx], XC.at[step, 1 - sz, 1 - sx])
            elif kind[:2] == "yx":
                part = int(kind[2])
                pair = (YX.at[step, sy, sx, part], YXR.at[step, 1 - sy, 1 - sx, part])
            else:
                low, high = spans[step][kind[1]]
                if kind[0] == "y":
                    pair = (YP.at[step, sy, low:high], YR.at[step, 1 - sy, low + 1:high + 1])
                else:
                    pair = (
                        U.at[step, :, low + 2:high + 2, tile, body_rows],
                        XR.at[step, 1 - sx, :, low:high],
                    )
            return pltpu.make_async_remote_copy(
                src_ref=pair[0],
                dst_ref=pair[1],
                send_sem=send_sem.at[0],
                recv_sem=recv_sem.at[slot(step, kind)],
                device_id=neighbour(d),
                device_id_type=MESH,
            )

        def each(step, kinds, sign, action):
            for name in kinds:
                for kind, d in KINDS:
                    if kind == name and feasible(d):
                        @pl.when(inside(d, sign))
                        def _():
                            action(message(step, kind, d))

        def settle(tiles, sem):
            if tiles:
                pltpu.make_async_copy(W.at[0:tiles], W.at[0:tiles], sem).wait()

        def settle_messages(steps, kinds, sem):
            for number in itertools.product(*[
                (0,) if n == 1 else (1,) if n == 2 else (1, 2) for n in sizes
            ]):
                here = None
                for m, n, k in zip(me, sizes, number):
                    if n > 2:
                        both = jnp.logical_and(m > 0, m < n - 1)
                        ok = both if k == 2 else jnp.logical_not(both)
                        here = ok if here is None else jnp.logical_and(here, ok)
                tiles = sum(group_tiles(t, kinds(t), number, Z, R, L) for t in steps)

                def wait():
                    settle(tiles, sem)

                if here is None:
                    wait()
                else:
                    pl.when(here)(wait)

        def send(step, *kinds):
            each(step, kinds, 1, lambda copy: copy.start())

        def receive(step, *kinds):
            settle_messages((step,), lambda _: kinds, recv_sem.at[slot(step, kinds[0])])

        def pack_plane(step, z, save):
            for side, firsts in (
                (0, [TOP - 2 * f for f in range(4)]),
                (1, [END - 2 - 2 * f for f in range(3)] + [END - 7]),
            ):
                for l in range(L):
                    rows = [U[step, f, z + 2, l, at:at + 8, :] for f, at in enumerate(firsts)]
                    save(side, l, jnp.where(
                        row8t < 2, rows[0],
                        jnp.where(row8t < 4, rows[1], jnp.where(row8t < 6, rows[2], rows[3])),
                    ))

        def pack_y(step, part):
            for z in groups[step][part]:
                def save(side, l, value):
                    YP[step, side, z, :, 128 * l:128 * l + 128] = value

                pack_plane(step, z, save)
            for side in range(2):
                for sx in range(2):
                    tile = jnp.zeros((8, 128), F32)
                    for z in groups[step][part]:
                        value = YP[step, side, z, :, (C - 128) * sx:(C - 128) * sx + 128]
                        tile = jnp.where(lane8 == z, roll(value, z + sx, 1), tile)
                    YX[step, side, sx, part] = tile

        def pack_corners(step):
            for sz, z in ((0, 0), (1, Z - 1)):
                for sx in range(2):
                    tiles = [
                        roll(U[step, f, z + 2, (L - 1) * sx, body_rows, :], f + sx, 1)
                        for f in range(3)
                    ]
                    XS[step, sz, sx] = jnp.where(
                        lane_r == 0, tiles[0], jnp.where(lane_r == 1, tiles[1], tiles[2])
                    )

                def save(side, l, value):
                    YZ[step, side, sz, :, 128 * l:128 * l + 128] = value

                pack_plane(step, z, save)

        def unpack_x(step, z):
            for f in range(4):
                U[step, f, z + 2, L, body_rows, :] = jnp.where(
                    lane_r < 64, XR[step, 1, f, z], XR[step, 0, f, z]
                )

        def unpack_zx(step):
            for sz, z in ((0, -1), (1, Z)):
                for f in range(3):
                    U[step, f, z + 2, L, body_rows, :] = jnp.where(
                        lane_r < 64, roll(XC[step, sz, 1], -f, 1), roll(XC[step, sz, 0], 127 - f, 1)
                    )

        def put_rows(step, z, l, low, high, fields):
            for f in range(fields):
                if f < 3:
                    U[step, f, z + 2, l, TOP - 2:TOP, :] = low[2 * f:2 * f + 2]
                    U[step, f, z + 2, l, END:END + 2, :] = high[2 * f:2 * f + 2]
                else:
                    U[step, f, z + 2, l, TOP - 1:TOP, :] = low[6:7]
                    U[step, f, z + 2, l, END:END + 1, :] = high[6:7]

        def unpack_y(step, z, fields):
            for l in range(L):
                low, high = [YR[step, side, z + 1, :, 128 * l:128 * l + 128] for side in range(2)]
                put_rows(step, z, l, low, high, fields)

        def unpack_yx(step, part):
            for z in groups[step][part]:
                low, high = [
                    jnp.where(
                        lane8 < 64, roll(YXR[step, sy, 1, part], -z, 1),
                        roll(YXR[step, sy, 0, part], 127 - z, 1),
                    )
                    for sy in range(2)
                ]
                put_rows(step, z, L, low, high, 3)

        def take(step, f, z, row, tiles):
            parts = [U[step, f, z, l, row:row + 8, :] for l in range(tiles)]
            return jnp.concatenate(parts, axis=1)

        def slope_z(step, f, z, row, tiles):
            return take(step, f, z + 3, row, tiles) - take(step, f, z + 1, row, tiles)

        def slope_y(step, f, z, row, tiles):
            return take(step, f, z + 2, row + 1, tiles) - take(step, f, z + 2, row - 1, tiles)

        def beside(value, tiles):
            parts = [value[:, 128 * l:128 * l + 128] for l in range(L + 1)]
            after, before = [], []
            for l in range(tiles):
                after.append(roll(jnp.where(lane8 == 0, parts[(l + 1) % (L + 1)], parts[l]), -1, 1))
                before.append(roll(jnp.where(lane8 == 127, parts[l - 1], parts[l]), 1, 1))
            return jnp.concatenate(after, axis=1), jnp.concatenate(before, axis=1)

        def along_x(value, tiles):
            after, before = beside(value, tiles)
            return after - before

        def slope_x(step, f, z, row):
            return along_x(take(step, f, z + 2, row, L + 1), L)

        def gain(step, z, row, tiles):
            keep = 1.0 - take(step, 3, z + 2, row, tiles)
            return (0.5 * TIME_DISP) * (keep * keep + RESIDUAL_STIFF)

        def store(step, f, z, row, value):
            if step == 0:
                for l in range(L):
                    U[1, f, z + 2, l, row:row + 8, :] = value[:, 128 * l:128 * l + 128]
            elif f < 3:
                moved_ref[f, z, row - TOP:row - TOP + 8, :] = value
            else:
                damage_ref[z, row - TOP:row - TOP + 8, :] = value

        core_rows = range(TOP, END, 8)

        def ends(step, z):
            for row in core_rows:
                gz = [slope_z(step, f, z, row, L) for f in range(3)]
                gy0, gy1 = slope_y(step, 0, z, row, L), slope_y(step, 1, z, row, L)
                gx0, gx2 = slope_x(step, 0, z, row), slope_x(step, 2, z, row)
                g = gain(step, z, row, L)
                h = 0.5 * g
                at = slice(row - TOP, row - TOP + 8)
                TZ[z + 1, 0, at] = g * (gz[0] + 0.75 * (gz[0] + gy1 + gx2))
                TZ[z + 1, 1, at] = h * (gz[1] + gy0)
                TZ[z + 1, 2, at] = h * (gz[2] + gx0)

        def hurt(step, z, row, gz0, gy1, gx2, a01, a02, a12):
            energy = energy_of(gz0, gy1, gx2, a01, a02, a12)
            dx = take(step, 3, z + 2, row, L + 1)
            dc = dx[:, 0:C]
            after, before = beside(dx, L)
            lap = (
                take(step, 3, z + 3, row, L) + take(step, 3, z + 1, row, L)
                + take(step, 3, z + 2, row + 1, L) + take(step, 3, z + 2, row - 1, L)
                + (after + before)
                - 7.0 * dc
            )
            store(step, 3, z, row, dc + TIME_DAMAGE * (
                0.5 * (1.0 - dc) * energy + tough[z, row - TOP:row - TOP + 8, :] * lap
            ))

        def damage(step, z):
            for row in core_rows:
                gz = [slope_z(step, f, z, row, L) for f in range(3)]
                gy = [slope_y(step, f, z, row, L) for f in range(3)]
                gx = [slope_x(step, f, z, row) for f in range(3)]
                hurt(
                    step, z, row, gz[0], gy[1], gx[2],
                    gz[1] + gy[0], gz[2] + gx[0], gy[2] + gx[1],
                )

        def put_y(row, values):
            for i in range(3):
                for l in range(L):
                    TY[i, l, row:row + 8, :] = values[i][:, 128 * l:128 * l + 128]

        def force(step, z, with_damage):
            for row in (TOP - 8, END):
                gy = [slope_y(step, f, z, row, L) for f in range(3)]
                gx1, gx2 = [slope_x(step, f, z, row) for f in (1, 2)]
                gz0, gz1 = [slope_z(step, f, z, row, L) for f in (0, 1)]
                g = gain(step, z, row, L)
                h = 0.5 * g
                put_y(row, [
                    h * (gz1 + gy[0]), g * (gy[1] + 0.75 * (gz0 + gy[1] + gx2)), h * (gy[2] + gx1)
                ])

            def close(row, waiting):
                for i in range(3):
                    change = jnp.concatenate(
                        [TY[i, l, row + 1:row + 9, :] - TY[i, l, row - 1:row + 7, :] for l in range(L)],
                        axis=1,
                    )
                    store(step, i, z, row, waiting[i] + change)

            waiting = None
            for row in core_rows:
                wide = L + 1
                now = [take(step, f, z + 2, row, wide) for f in range(3)]
                gz = [slope_z(step, f, z, row, wide) for f in range(3)]
                gy = [slope_y(step, f, z, row, wide) for f in range(3)]
                gx = [along_x(v, wide) for v in now]
                g = gain(step, z, row, wide)
                h = 0.5 * g
                lam = 0.75 * (gz[0] + gy[1] + gx[2])
                a01 = (gz[1] + gy[0])[:, 0:C]
                a02 = gz[2] + gx[0]
                a12 = gy[2] + gx[1]
                t01, t02, t12 = h[:, 0:C] * a01, h * a02, h * a12
                put_y(row, [t01, (g * (gy[1] + lam))[:, 0:C], t12[:, 0:C]])
                at = slice(row - TOP, row - TOP + 8)
                TZ[z + 1, 0, at] = (g * (gz[0] + lam))[:, 0:C]
                TZ[z + 1, 1, at] = t01
                TZ[z + 1, 2, at] = t02[:, 0:C]
                ready = [
                    now[i][:, 0:C] + along_x(t, L)
                    for i, t in enumerate((t02, t12, g * (gx[2] + lam)))
                ]
                if waiting is not None:
                    close(row - 8, waiting)
                waiting = ready
                if with_damage:
                    hurt(
                        step, z, row, gz[0][:, 0:C], gy[1][:, 0:C], gx[2][:, 0:C],
                        a01, a02[:, 0:C], a12[:, 0:C],
                    )
            close(END - 8, waiting)

        def finish(step, z):
            for i in range(3):
                for l in range(L):
                    lanes = slice(128 * l, 128 * l + 128)
                    U[1, i, z + 2, l, body_rows, :] = U[1, i, z + 2, l, body_rows, :] + (
                        TZ[z + 2, i, :, lanes] - TZ[z, i, :, lanes]
                    )

        def finish_pool(z, row):
            means = []
            for i in range(3):
                value = moved_ref[i, z] + (TZ[z + 2, i] - TZ[z, i])
                moved_ref[i, z] = value
                folded = value[:, 0:128]
                for cut in range(128, C, 128):
                    folded = folded + value[:, cut:cut + 128]
                means.append(jnp.sum(folded, axis=1, keepdims=True) * (1.0 / C))
            pooled_t[row:row + R, :] = jnp.where(
                lane_r == 0, means[0], jnp.where(lane_r == 1, means[1], means[2])
            )

        def pooled(rows_here):
            value = pooled_t[0:rows_here, :].T[0:8].astype(jnp.bfloat16)
            return jnp.concatenate([value, value], axis=1)

        settle(2 * 3 * 2 * L * R // 8, in_sem.at[0])
        with scope("barrier"):
            pl.semaphore_wait(barrier, met)
        send(0, "zu")
        pack_corners(0)
        send(0, "zx", "zy")
        crack_load.wait()

        def label(z, carry):
            for l in range(L):
                U[0, 3, z + 2, l, body_rows, :] = DAMAGE_LEVEL * crack[
                    z, :, 128 * l:128 * l + 128
                ].astype(F32)
            return carry

        lax.fori_loop(0, Z, label, 0)
        settle(3 * (Z - 4) * L * R // 8, in_sem.at[4])
        with scope("pack"):
            pack_y(0, 0)
            send(0, "y0", "yx0", "x0", "zd", "zs")
            for item in [tough_load, *weight_loads]:
                item.start()
        for side, sign in ((0, -1), (1, 1)):
            clear((sign, 0, 0), clear_z(side))
            clear((0, sign, 0), clear_y(side))
            clear((0, 0, sign), clear_x(side))

        cell_load.wait()
        base = me[0] * Z * (R * n_pencil) + me[1] * R
        row_id = lax.broadcasted_iota(jnp.int32, (R, 512), 0) * n_comp

        def choose(part, z, row):
            start = (base + z * (R * n_pencil)) * n_comp + me[2]
            for s in range(0, sensors, 512):
                hit = row_id == cell_ref[:, s:s + 512] - start
                weight[part, row:row + R, s:s + 512] = jnp.where(hit, POINT_GAIN, 0.0).astype(
                    jnp.bfloat16
                )

        with scope("choose"):
            for k, z in enumerate((0, 1, Z - 2, Z - 1)):
                choose(0, z, rim + k * R)
            for z in range(2, Z - 2):
                choose(1, z, inner + (z - 2) * R)
            tough_load.wait()
        with scope("waitx"):
            receive(0, "x0")
        with scope("unpx"):
            loop(0, Z, lambda z: unpack_x(0, z))
        with scope("waity"):
            receive(0, "y0", "yx0")
        with scope("unpy"):
            loop(0, Z, lambda z: unpack_y(0, z, 4))
            unpack_yx(0, 0)
        with scope("body"):
            loop(0, 2, lambda k: force(0, 2 + k * (Z - 5), True))
            loop(0, 2, lambda k: force(0, 1 + k * (Z - 3), False))
        with scope("waitza"):
            receive(0, *EDGE)
        with scope("edge"):
            unpack_zx(0)
            for z in (-1, Z):
                unpack_y(0, z, 3)
            loop(0, 2, lambda k: force(0, k * (Z - 1), False))
            loop(0, 2, lambda k: finish(0, 1 + k * (Z - 3)))
        send(1, "zs")
        with scope("body2"):
            loop(3, Z - 3, lambda z: force(0, z, True))
            loop(2, Z - 2, lambda z: finish(0, z))
            pack_y(1, 0)
            send(1, "y0", "yx0", "x0")
            loop(0, 2, lambda k: damage(0, 1 + k * (Z - 3)))
        with scope("waitzb"):
            receive(0, *REST)
        with scope("ends"):
            loop(0, 2, lambda k: ends(0, k * (Z + 1) - 1))
            loop(0, 2, lambda k: finish(0, k * (Z - 1)))
        pack_corners(1)
        send(1, "zu", "zx", "zy")
        with scope("damage"):
            loop(0, 2, lambda k: damage(0, k * (Z - 1)))
        send(1, "zd")
        with scope("pack2"):
            pack_y(1, 1)
            send(1, "y1", "y2", "yx1", "x1", "x2")

        with scope("waitx"):
            receive(1, "x0")
            loop(2, Z - 2, lambda z: unpack_x(1, z))
        with scope("waity"):
            receive(1, "y0", "yx0")
            loop(2, Z - 2, lambda z: unpack_y(1, z, 4))
            unpack_yx(1, 0)
        with scope("body"):
            loop(3, Z - 3, lambda z: force(1, z, False))
        with scope("waitxy"):
            receive(1, "x1", "x2", "y1", "y2", "yx1")
        with scope("unpxy"):
            for z in (0, 1, Z - 2, Z - 1):
                unpack_x(1, z)
                unpack_y(1, z, 4)
            unpack_yx(1, 1)
        with scope("body2"):
            loop(0, 2, lambda k: force(1, 1 + k * (Z - 3), False))
            loop(0, 2, lambda k: force(1, 2 + k * (Z - 5), False))
        with scope("pooli"):
            for z in range(2, Z - 2):
                finish_pool(z, (z - 2) * R)
        with scope("doti"):
            settle(Z * R * sensors * 2 // 4096, in_sem.at[5])
            lhs = pooled(inner)
            for cut in range(0, sensors, 256):
                acc[:, cut:cut + 256] = jnp.dot(
                    lhs, weight[1, 0:2 * inner, cut:cut + 256], preferred_element_type=F32
                )
        with scope("waitz"):
            receive(1, *REST, *EDGE)
        with scope("edge"):
            unpack_zx(1)
            for z in (-1, Z):
                unpack_y(1, z, 3)
            loop(0, 2, lambda k: force(1, k * (Z - 1), False))
            loop(0, 2, lambda k: ends(1, k * (Z + 1) - 1))
        with scope("poole"):
            for k, z in enumerate((0, 1, Z - 2, Z - 1)):
                finish_pool(z, k * R)

        def spread(stop, function):
            if stop <= 16:
                for k in range(stop):
                    function(k)
            else:
                loop(0, stop, function)

        def owner(q):
            return {"slab": first_slab + q // n_pencil, "pencil": q % n_pencil, "comp": n_comp - 1}

        def owned_by(q):
            return jnp.logical_and(mine == q, me[2] == n_comp - 1)

        def scatter(q):
            return pltpu.make_async_remote_copy(
                src_ref=partial.at[q], dst_ref=RB.at[flat],
                send_sem=send_sem.at[1], recv_sem=recv_sem.at[8],
                device_id=owner(q), device_id_type=MESH,
            )

        def landed(ref, sem):
            pltpu.make_async_copy(ref, ref, sem).wait()

        def gather(q, k):
            return pltpu.make_async_remote_copy(
                src_ref=GB.at[q], dst_ref=GB.at[q],
                send_sem=send_sem.at[2], recv_sem=recv_sem.at[9],
                device_id=device(k), device_id_type=MESH,
            )

        def unless(same, function):
            @pl.when(jnp.logical_not(same))
            def _():
                function()

        mine = (me[0] - first_slab) * n_pencil + me[1]
        owning = jnp.logical_and(
            me[2] == n_comp - 1, jnp.logical_and(mine >= 0, mine < owners)
        )
        with scope("dot"):
            lhs = pooled(rim)
            for cut in range(0, sensors, 256):
                value = acc[:, cut:cut + 256] + jnp.dot(
                    lhs, weight[0, 0:2 * rim, cut:cut + 256], preferred_element_type=F32
                )
                for low in (0, 128):
                    for c in range(3):
                        partial[(cut + low) // piece, c, (cut + low) % piece // 128] = (
                            value[c, low:low + 128]
                        )
        with scope("rssend"):
            for q in range(owners):
                unless(owned_by(q), lambda: scatter(q).start())

        with scope("damage"):
            loop(0, Z, lambda z: damage(1, z))

        @pl.when(owning)
        def _():
            with scope("waitrs"):
                landed(RB.at[0:count - 1], recv_sem.at[8])
            RB[flat] = partial[mine]
            if count <= 16:
                total = RB[0]
                for k in range(1, count):
                    total = total + RB[k]
            else:
                total = lax.fori_loop(1, count, lambda k, t: t + RB[k], RB[0])
            GB[mine] = total
            spread(count, lambda k: unless(flat == k, lambda: gather(mine, k).start()))

        with scope("waitag"):
            @pl.when(owning)
            def _():
                if owners > 1:
                    landed(GB.at[0:owners - 1], recv_sem.at[9])

            @pl.when(jnp.logical_not(owning))
            def _():
                landed(GB.at[0:owners], recv_sem.at[9])

        for q in range(owners):
            for c in range(3):
                for k in range(strips):
                    low = q * piece + 128 * k
                    read_ref[c, low:low + 128] = GB[q, c, k]
        with scope("sends"):
            settle_messages((0, 1), lambda t: SENT[t], send_sem.at[0])

            @pl.when(owning)
            def _():
                if owners > 1:
                    landed(partial.at[0:owners - 1], send_sem.at[1])
                landed(RB.at[0:count - 1], send_sem.at[2])

            @pl.when(jnp.logical_not(owning))
            def _():
                landed(partial.at[0:owners], send_sem.at[1])

    return kernel


def emit(moved_ref, damage_ref, read_ref, moved_hbm, damage_hbm, read_hbm, sem):
    copies = [
        pltpu.make_async_copy(moved_ref, moved_hbm, sem.at[0]),
        pltpu.make_async_copy(damage_ref, damage_hbm, sem.at[1]),
        pltpu.make_async_copy(read_ref, read_hbm, sem.at[2]),
    ]
    for copy in copies:
        copy.start()
    for copy in copies:
        copy.wait()


def solution(mesh):
    sizes = tuple(mesh.shape[a] for a in AXES)
    n_slab = sizes[0]
    count = sizes[0] * sizes[1] * sizes[2]

    def local(u_start, toughness, crack_label, obs_weight, sensor_cell):
        Z, R, C = toughness.shape
        S = sensor_cell.shape[0]
        first_slab = max(n_slab // 2 - 1, 0)
        owners = min(2, n_slab) * sizes[1]
        while S % (owners * 256):
            owners -= 1
        piece = S // owners
        rim, inner = 4 * R, (Z - 4) * R
        most = max(
            Z * R * S * 2 // 4096,
            sum(group_tiles(t, SENT[t], (2, 2, 2), Z, R, C // 128) for t in range(2)),
        )
        any_spec = pl.BlockSpec(memory_space=pltpu.HBM)
        vmem_spec = pl.BlockSpec(memory_space=pltpu.VMEM)
        dma = pltpu.SemaphoreType.DMA
        shapes = (
            jax.ShapeDtypeStruct((3, Z, R, C), F32),
            jax.ShapeDtypeStruct((Z, R, C), F32),
            jax.ShapeDtypeStruct((3, S), F32),
        )
        outs = pl.pallas_call(
            make_kernel(Z, R, C, S, sizes, first_slab, owners),
            out_shape=shapes,
            in_specs=[any_spec] * 5,
            out_specs=[vmem_spec] * 3,
            scratch_shapes=[
                pltpu.VMEM((2, 4, Z + 4, C // 128 + 1, R + 32, 128), F32),
                pltpu.VMEM((2, 2, 4, Z, R, 128), F32),
                pltpu.VMEM((2, 2, 2, R, 128), F32),
                pltpu.VMEM((2, 2, 2, R, 128), F32),
                pltpu.VMEM((2, 2, Z + 2, 8, C), F32),
                pltpu.VMEM((2, 2, Z, 8, C), F32),
                pltpu.VMEM((2, 2, 2, 8, C), F32),
                pltpu.VMEM((2, 2, 2, 2, 8, 128), F32),
                pltpu.VMEM((2, 2, 2, 2, 8, 128), F32),
                pltpu.VMEM((Z + 2, 3, R, C), F32),
                pltpu.VMEM((3, C // 128, R + 32, 128), F32),
                pltpu.VMEM((most, 8, 128), F32),
                pltpu.VMEM((Z, R, C), F32),
                pltpu.VMEM((Z, R, C), jnp.int32),
                pltpu.VMEM((2, 2 * max(rim, inner), S), jnp.bfloat16),
                pltpu.VMEM((1, S), jnp.int32),
                pltpu.VMEM((max(rim, inner), 128), F32),
                pltpu.VMEM((8, S), F32),
                pltpu.VMEM((owners, 3, piece // 128, 128), F32),
                pltpu.VMEM((count, 3, piece // 128, 128), F32),
                pltpu.VMEM((owners, 3, piece // 128, 128), F32),
                dma((6,)),
                dma((3,)),
                dma((10,)),
            ],
            compiler_params=pltpu.CompilerParams(
                collective_id=0, has_side_effects=True, vmem_limit_bytes=40 * 1024 * 1024
            ),
            name="fracture",
        )(
            *[
                pltpu.with_memory_space_constraint(x, pltpu.HBM)
                for x in (
                    u_start, toughness, crack_label, obs_weight.reshape(Z * R, S),
                    sensor_cell.reshape(1, S),
                )
            ],
        )
        return pl.pallas_call(
            emit,
            out_shape=shapes,
            in_specs=[vmem_spec] * 3,
            out_specs=[any_spec] * 3,
            scratch_shapes=[dma((3,))],
            name="emit",
        )(*[pltpu.with_memory_space_constraint(x, pltpu.VMEM) for x in outs])

    return jax.shard_map(
        local,
        mesh=mesh,
        in_specs=(
            P(None, ("groups", "slab"), "pencil", "comp"),
            P(("groups", "slab"), "pencil", "comp"),
            P(("groups", "slab"), "pencil", "comp"),
            P("slab", "pencil", "comp", None),
            P(),
        ),
        out_specs=(
            P(None, ("groups", "slab"), "pencil", "comp"),
            P(("groups", "slab"), "pencil", "comp"),
            P(None, "groups"),
        ),
        check_vma=False,
    )
```

```python
import itertools

import jax
import jax.numpy as jnp
import numpy as np
from jax import lax
from jax.experimental import pallas as pl
from jax.experimental.pallas import tpu as pltpu
from jax.sharding import PartitionSpec as P

RESIDUAL_STIFF = 0.001
TIME_DISP = 0.15
TIME_DAMAGE = 0.08
DAMAGE_LEVEL = 0.45
POINT_GAIN = 8.0
AXES = ("slab", "pencil", "comp")
MESH = pl.DeviceIdType.MESH
F32 = jnp.float32


def third_angle_poly():
    nodes = 0.5 + 0.5 * np.cos(np.pi * (np.arange(200) + 0.5) / 200)
    fit = np.polynomial.chebyshev.Chebyshev.fit(
        nodes, np.cos(np.arccos(nodes) / 3.0), 8, domain=[0.0, 1.0]
    )
    return [float(c) for c in fit.convert(kind=np.polynomial.Polynomial).coef]


POLY = third_angle_poly()

DIRECTIONS = [
    d for d in itertools.product((-1, 0, 1), repeat=3) if 1 <= sum(map(abs, d)) <= 2
]
ALONG_Z = [d for d in DIRECTIONS if d[0] and not d[1] and not d[2]]
ALONG_Y = [d for d in DIRECTIONS if d[1] and not d[0] and not d[2]]
ALONG_X = [d for d in DIRECTIONS if d[2] and not d[0] and not d[1]]
DIAG_ZY = [d for d in DIRECTIONS if d[0] and d[1]]
DIAG_ZX = [d for d in DIRECTIONS if d[0] and d[2]]
DIAG_YX = [d for d in DIRECTIONS if d[1] and d[2]]
KINDS = (
    [("zu", d) for d in ALONG_Z] + [("zy", d) for d in DIAG_ZY] + [("zx", d) for d in DIAG_ZX]
    + [("zd", d) for d in ALONG_Z] + [("zs", d) for d in ALONG_Z]
    + [(k, d) for k in ("y0", "y1", "y2") for d in ALONG_Y]
    + [(k, d) for k in ("yx0", "yx1") for d in DIAG_YX]
    + [(k, d) for k in ("x0", "x1", "x2") for d in ALONG_X]
)
EDGE = ("zu", "zy", "zx")
REST = ("zd", "zs")


def energy_of(g0, g1, g2, a01, a02, a12):
    trace = g0 + g1 + g2
    mean = trace * (1.0 / 3.0)
    d0, d1, d2 = g0 - mean, g1 - mean, g2 - mean
    q01, q02, q12 = a01 * a01, a02 * a02, a12 * a12
    d01 = d0 * d1
    p2 = (d0 * d0 + d1 * d1 + d01) * (1.0 / 3.0) + (q01 + q02 + q12) * (1.0 / 12.0)
    inv = lax.rsqrt(jnp.maximum(p2, 1e-36))
    p = p2 * inv
    det = d01 * d2 + 0.25 * (a01 * a02 * a12 - d0 * q12 - d1 * q02 - d2 * q01)
    half_det = ((det * inv) * inv) * (0.5 * inv)
    r = jnp.minimum(jnp.abs(half_det), 1.0)
    c = jnp.full_like(r, POLY[-1])
    for coefficient in POLY[-2::-1]:
        c = c * r + coefficient
    tc = p * c
    t = jnp.where(half_det < 0.0, -tc, tc)
    s2 = jnp.maximum(1.0 - c * c, 0.0)
    delta = p * (s2 * lax.rsqrt(jnp.maximum(s2, 1e-30))) * float(np.sqrt(3.0))
    f1 = jnp.maximum(mean + 2.0 * t, 0.0)
    f2 = jnp.maximum(mean - t + delta, 0.0)
    f3 = jnp.maximum(mean - t - delta, 0.0)
    ft = jnp.maximum(trace, 0.0)
    return 0.75 * ft * ft + f1 * f1 + f2 * f2 + f3 * f3


def message_tiles(kind, step, Z, R, L):
    if kind in ("zu", "zs"):
        return 3 * L * R // 8
    if kind == "zd":
        return L * R // 8
    if kind == "zx":
        return 1
    if kind == "zy":
        return L
    if kind[:2] == "yx":
        return 1
    planes = 1 if kind[1] != "0" else Z - 2 if step else Z
    return planes * L if kind[0] == "y" else planes * 4 * R // 8


SENT = [
    ("zu", "zx", "zy", "zd", "zs", "y0", "yx0", "x0"),
    ("zu", "zx", "zy", "zd", "zs", "y0", "yx0", "x0", "y1", "y2", "yx1", "x1", "x2"),
]


def group_tiles(step, kinds, met, Z, R, L):
    total = 0
    for kind in kinds:
        number = message_tiles(kind, step, Z, R, L)
        axes = [a for a, name in enumerate("zyx") if name in kind[:2]]
        for a in axes if kind[:2] in ("zx", "zy", "yx") else axes[:1]:
            number *= met[a]
        total += number
    return total


def make_kernel(planes, rows, columns, sensors, sizes, first_slab, owners):
    n_slab, n_pencil, n_comp = sizes
    count = n_slab * n_pencil * n_comp
    Z, R, C = planes, rows, columns
    piece = sensors // owners
    strips = piece // 128
    L = C // 128
    TOP = 16
    END = TOP + R
    body_rows = slice(TOP, END)
    rim = 4 * R
    spans = {
        0: {"0": (0, Z)},
        1: {"0": (1, Z - 1), "1": (0, 1), "2": (Z - 1, Z)},
    }
    groups = {0: [range(Z)], 1: [range(1, Z - 1), [0, Z - 1]]}
    near = n_slab <= 4 and n_pencil <= 2 and n_comp <= 2

    def scope(name):
        return jax.named_scope(name)

    def kernel(u_hbm, tough_hbm, crack_hbm, weight_hbm, cell_hbm,
               moved_ref, damage_ref, read_ref,
               U, XR, XS, XC, YR, YP, YZ, YX, YXR, TZ, TY, W, tough, crack, weight, cell_ref, pooled_t, acc,
               partial, RB, GB,
               in_sem, send_sem, recv_sem):
        me = [lax.axis_index(a) for a in AXES]
        flat = (me[0] * n_pencil + me[1]) * n_comp + me[2]

        def device(index):
            return {
                "slab": index // (n_pencil * n_comp),
                "pencil": (index // n_comp) % n_pencil,
                "comp": index % n_comp,
            }

        def u_load(k, low, high):
            return [
                pltpu.make_async_copy(
                    u_hbm.at[:, low:high, :, 128 * l:128 * l + 128],
                    U.at[0, 0:3, low + 2:high + 2, l, body_rows, :],
                    in_sem.at[4 if k == 2 else 0],
                )
                for l in range(L)
            ]

        edge_loads = u_load(0, 0, 2) + u_load(1, Z - 2, Z)
        inner_loads = u_load(2, 2, Z - 2)
        crack_load = pltpu.make_async_copy(crack_hbm, crack, in_sem.at[1])
        tough_load = pltpu.make_async_copy(tough_hbm, tough, in_sem.at[2])
        cell_load = pltpu.make_async_copy(cell_hbm, cell_ref, in_sem.at[3])
        inner = Z * R - rim
        weight_loads = [
            pltpu.make_async_copy(weight_hbm.at[0:rim // 2], weight.at[0, 0:rim // 2], in_sem.at[5]),
            pltpu.make_async_copy(
                weight_hbm.at[Z * R - rim // 2:Z * R], weight.at[0, rim // 2:rim], in_sem.at[5]),
            pltpu.make_async_copy(
                weight_hbm.at[rim // 2:Z * R - rim // 2], weight.at[1, 0:inner], in_sem.at[5]),
        ]
        for item in edge_loads:
            item.start()

        barrier = pltpu.get_barrier_semaphore()

        def inside(d, sign):
            ok = None
            for m, o, n in zip(me, d, sizes):
                if o:
                    here = m + 1 < n if sign * o > 0 else m >= 1
                    ok = here if ok is None else jnp.logical_and(ok, here)
            return ok

        def feasible(d):
            return all(n > 1 for o, n in zip(d, sizes) if o)

        def neighbour(d):
            return {a: m + o for a, m, o in zip(AXES, me, d)}

        met = 0
        if near:
            for d in DIRECTIONS:
                if feasible(d):
                    @pl.when(inside(d, 1))
                    def _():
                        pl.semaphore_signal(
                            barrier, inc=1, device_id=neighbour(d), device_id_type=MESH
                        )

                    met = met + inside(d, 1).astype(jnp.int32)
        else:
            def greet(k, carry):
                pl.semaphore_signal(
                    barrier, inc=1, device_id=device((flat + k) % count), device_id_type=MESH
                )
                return carry

            lax.fori_loop(1, count, greet, 0)
            met = count - 1

        for item in [crack_load, *inner_loads, cell_load]:
            item.start()

        def clear(d, write):
            if feasible(d):
                @pl.when(jnp.logical_not(inside(d, 1)))
                def _():
                    write()
            else:
                write()

        def clear_z(up):
            def write():
                for step in range(2):
                    for z in ((Z + 2, Z + 3) if up else (0, 1)):
                        U[step, :, z, 0:L, body_rows] = jnp.zeros((4, L, R, 128), F32)
                XC[:, up] = jnp.zeros((2, 2, 8, 128), F32)
                for step in range(2):
                    for side in range(2):
                        YR[step, side, (Z + 1) * up] = jnp.zeros((8, C), F32)
            return write

        def clear_x(right):
            def write():
                def one(k, carry):
                    XR[k // (4 * Z), right, (k // Z) % 4, k % Z] = jnp.zeros((R, 128), F32)
                    return carry

                lax.fori_loop(0, 8 * Z, one, 0)
                XC[:, :, right] = jnp.zeros((2, 2, 8, 128), F32)
                YXR[:, :, right] = jnp.zeros((2, 2, 2, 8, 128), F32)
            return write

        def clear_y(up):
            def write():
                YR[:, up] = jnp.zeros((2, Z + 2, 8, C), F32)
                YXR[:, up] = jnp.zeros((2, 2, 2, 8, 128), F32)
            return write

        core_rows = range(TOP, END, 8)
        row8t = lax.broadcasted_iota(jnp.int32, (8, 128), 0)
        lane8 = lax.broadcasted_iota(jnp.int32, (8, 128), 1)
        lane_r = lax.broadcasted_iota(jnp.int32, (R, 128), 1)

        def roll(value, shift, axis):
            shift = shift % value.shape[axis]
            return pltpu.roll(value, shift, axis) if shift else value

        def loop(start, stop, function):
            def one(z, carry):
                function(z)
                return carry

            lax.fori_loop(start, stop, one, 0)

        def slot(step, kind):
            if step == 0:
                return 0 if kind in EDGE else 1 if kind in REST else 2 if kind[0] == "x" else 3
            if kind[0] == "z":
                return 4
            if kind[-1] == "0":
                return 5 if kind[0] == "x" else 6
            return 10 if kind[0] == "x" else 7

        def message(step, kind, d):
            dz, dy, dx = d
            sz, sy, sx = (dz + 1) // 2, (dy + 1) // 2, (dx + 1) // 2
            tile = L - 1 if dx > 0 else 0
            edge = Z - 1 if dz > 0 else 0
            halo = 0 if dz > 0 else Z + 1
            if kind == "zu":
                pair = (
                    U.at[step, 0:3, edge + 2, 0:L, body_rows], U.at[step, 0:3, halo + 1, 0:L, body_rows]
                )
            elif kind == "zs":
                pair = (
                    U.at[step, 0:3, Z if dz > 0 else 3, 0:L, body_rows],
                    U.at[step, 0:3, 0 if dz > 0 else Z + 3, 0:L, body_rows],
                )
            elif kind == "zd":
                pair = (U.at[step, 3, edge + 2, 0:L, body_rows], U.at[step, 3, halo + 1, 0:L, body_rows])
            elif kind == "zy":
                pair = (YZ.at[step, sy, sz], YR.at[step, 1 - sy, halo])
            elif kind == "zx":
                pair = (XS.at[step, sz, sx], XC.at[step, 1 - sz, 1 - sx])
            elif kind[:2] == "yx":
                part = int(kind[2])
                pair = (YX.at[step, sy, sx, part], YXR.at[step, 1 - sy, 1 - sx, part])
            else:
                low, high = spans[step][kind[1]]
                if kind[0] == "y":
                    pair = (YP.at[step, sy, low:high], YR.at[step, 1 - sy, low + 1:high + 1])
                else:
                    pair = (
                        U.at[step, :, low + 2:high + 2, tile, body_rows],
                        XR.at[step, 1 - sx, :, low:high],
                    )
            return pltpu.make_async_remote_copy(
                src_ref=pair[0],
                dst_ref=pair[1],
                send_sem=send_sem.at[0],
                recv_sem=recv_sem.at[slot(step, kind)],
                device_id=neighbour(d),
                device_id_type=MESH,
            )

        def each(step, kinds, sign, action):
            for name in kinds:
                for kind, d in KINDS:
                    if kind == name and feasible(d):
                        @pl.when(inside(d, sign))
                        def _():
                            action(message(step, kind, d))

        def settle(tiles, sem):
            if tiles:
                pltpu.make_async_copy(W.at[0:tiles], W.at[0:tiles], sem).wait()

        def settle_messages(steps, kinds, sem):
            for number in itertools.product(*[
                (0,) if n == 1 else (1,) if n == 2 else (1, 2) for n in sizes
            ]):
                here = None
                for m, n, k in zip(me, sizes, number):
                    if n > 2:
                        both = jnp.logical_and(m > 0, m < n - 1)
                        ok = both if k == 2 else jnp.logical_not(both)
                        here = ok if here is None else jnp.logical_and(here, ok)
                tiles = sum(group_tiles(t, kinds(t), number, Z, R, L) for t in steps)

                def wait():
                    settle(tiles, sem)

                if here is None:
                    wait()
                else:
                    pl.when(here)(wait)

        def send(step, *kinds):
            each(step, kinds, 1, lambda copy: copy.start())

        def receive(step, *kinds):
            settle_messages((step,), lambda _: kinds, recv_sem.at[slot(step, kinds[0])])

        def pack_plane(step, z, save):
            for side, firsts in (
                (0, [TOP - 2 * f for f in range(4)]),
                (1, [END - 2 - 2 * f for f in range(3)] + [END - 7]),
            ):
                for l in range(L):
                    rows = [U[step, f, z + 2, l, at:at + 8, :] for f, at in enumerate(firsts)]
                    save(side, l, jnp.where(
                        row8t < 2, rows[0],
                        jnp.where(row8t < 4, rows[1], jnp.where(row8t < 6, rows[2], rows[3])),
                    ))

        def pack_y(step, part):
            for z in groups[step][part]:
                def save(side, l, value):
                    YP[step, side, z, :, 128 * l:128 * l + 128] = value

                pack_plane(step, z, save)
            for side in range(2):
                for sx in range(2):
                    tile = jnp.zeros((8, 128), F32)
                    for z in groups[step][part]:
                        value = YP[step, side, z, :, (C - 128) * sx:(C - 128) * sx + 128]
                        tile = jnp.where(lane8 == z, roll(value, z + sx, 1), tile)
                    YX[step, side, sx, part] = tile

        def pack_corners(step):
            for sz, z in ((0, 0), (1, Z - 1)):
                for sx in range(2):
                    tile = jnp.zeros((8, 128), F32)
                    for k, row in enumerate(core_rows):
                        for f in range(3):
                            value = U[step, f, z + 2, (L - 1) * sx, row:row + 8, :]
                            lane = 3 * k + f
                            tile = jnp.where(lane8 == lane, roll(value, lane + sx, 1), tile)
                    XS[step, sz, sx] = tile

                def save(side, l, value):
                    YZ[step, side, sz, :, 128 * l:128 * l + 128] = value

                pack_plane(step, z, save)

        def unpack_x(step, z):
            for f in range(4):
                U[step, f, z + 2, L, body_rows, :] = jnp.where(
                    lane_r < 64, XR[step, 1, f, z], XR[step, 0, f, z]
                )

        def unpack_zx(step):
            for sz, z in ((0, -1), (1, Z)):
                right, left = XC[step, sz, 1], XC[step, sz, 0]
                for k, row in enumerate(core_rows):
                    for f in range(3):
                        lane = 3 * k + f
                        U[step, f, z + 2, L, row:row + 8, :] = jnp.where(
                            lane8 < 64, roll(right, -lane, 1), roll(left, 127 - lane, 1)
                        )

        def put_rows(step, z, l, low, high, fields):
            for f in range(fields):
                if f < 3:
                    U[step, f, z + 2, l, TOP - 2:TOP, :] = low[2 * f:2 * f + 2]
                    U[step, f, z + 2, l, END:END + 2, :] = high[2 * f:2 * f + 2]
                else:
                    U[step, f, z + 2, l, TOP - 1:TOP, :] = low[6:7]
                    U[step, f, z + 2, l, END:END + 1, :] = high[6:7]

        def unpack_y(step, z, fields):
            for l in range(L):
                low, high = [YR[step, side, z + 1, :, 128 * l:128 * l + 128] for side in range(2)]
                put_rows(step, z, l, low, high, fields)

        def unpack_yx(step, part):
            for z in groups[step][part]:
                low, high = [
                    jnp.where(
                        lane8 < 64, roll(YXR[step, sy, 1, part], -z, 1),
                        roll(YXR[step, sy, 0, part], 127 - z, 1),
                    )
                    for sy in range(2)
                ]
                put_rows(step, z, L, low, high, 3)

        def take(step, f, z, row, tiles):
            parts = [U[step, f, z, l, row:row + 8, :] for l in range(tiles)]
            return jnp.concatenate(parts, axis=1)

        def slope_z(step, f, z, row, tiles):
            return take(step, f, z + 3, row, tiles) - take(step, f, z + 1, row, tiles)

        def slope_y(step, f, z, row, tiles):
            return take(step, f, z + 2, row + 1, tiles) - take(step, f, z + 2, row - 1, tiles)

        def beside(value, tiles):
            parts = [value[:, 128 * l:128 * l + 128] for l in range(L + 1)]
            after, before = [], []
            for l in range(tiles):
                after.append(roll(jnp.where(lane8 == 0, parts[(l + 1) % (L + 1)], parts[l]), -1, 1))
                before.append(roll(jnp.where(lane8 == 127, parts[l - 1], parts[l]), 1, 1))
            return jnp.concatenate(after, axis=1), jnp.concatenate(before, axis=1)

        def along_x(value, tiles):
            after, before = beside(value, tiles)
            return after - before

        def slope_x(step, f, z, row):
            return along_x(take(step, f, z + 2, row, L + 1), L)

        def gain(step, z, row, tiles):
            keep = 1.0 - take(step, 3, z + 2, row, tiles)
            return (0.5 * TIME_DISP) * (keep * keep + RESIDUAL_STIFF)

        def store(step, f, z, row, value):
            if step == 0:
                for l in range(L):
                    U[1, f, z + 2, l, row:row + 8, :] = value[:, 128 * l:128 * l + 128]
            elif f < 3:
                moved_ref[f, z, row - TOP:row - TOP + 8, :] = value
            else:
                damage_ref[z, row - TOP:row - TOP + 8, :] = value

        def ends(step, z):
            for row in core_rows:
                gz = [slope_z(step, f, z, row, L) for f in range(3)]
                gy0, gy1 = slope_y(step, 0, z, row, L), slope_y(step, 1, z, row, L)
                gx0, gx2 = slope_x(step, 0, z, row), slope_x(step, 2, z, row)
                g = gain(step, z, row, L)
                h = 0.5 * g
                at = slice(row - TOP, row - TOP + 8)
                TZ[z + 1, 0, at] = g * (gz[0] + 0.75 * (gz[0] + gy1 + gx2))
                TZ[z + 1, 1, at] = h * (gz[1] + gy0)
                TZ[z + 1, 2, at] = h * (gz[2] + gx0)

        def hurt(step, z, row, gz0, gy1, gx2, a01, a02, a12):
            energy = energy_of(gz0, gy1, gx2, a01, a02, a12)
            dx = take(step, 3, z + 2, row, L + 1)
            dc = dx[:, 0:C]
            after, before = beside(dx, L)
            lap = (
                take(step, 3, z + 3, row, L) + take(step, 3, z + 1, row, L)
                + take(step, 3, z + 2, row + 1, L) + take(step, 3, z + 2, row - 1, L)
                + (after + before)
                - 7.0 * dc
            )
            store(step, 3, z, row, dc + TIME_DAMAGE * (
                0.5 * (1.0 - dc) * energy + tough[z, row - TOP:row - TOP + 8, :] * lap
            ))

        def damage(step, z):
            for row in core_rows:
                gz = [slope_z(step, f, z, row, L) for f in range(3)]
                gy = [slope_y(step, f, z, row, L) for f in range(3)]
                gx = [slope_x(step, f, z, row) for f in range(3)]
                hurt(
                    step, z, row, gz[0], gy[1], gx[2],
                    gz[1] + gy[0], gz[2] + gx[0], gy[2] + gx[1],
                )

        def put_y(z, row, values):
            for i in range(3):
                for l in range(L):
                    TY[z, i, l, row:row + 8, :] = values[i][:, 128 * l:128 * l + 128]

        def outer_rows(step, z):
            for row in (TOP - 8, END):
                gy = [slope_y(step, f, z, row, L) for f in range(3)]
                gx1, gx2 = [slope_x(step, f, z, row) for f in (1, 2)]
                gz0, gz1 = [slope_z(step, f, z, row, L) for f in (0, 1)]
                g = gain(step, z, row, L)
                h = 0.5 * g
                put_y(z, row, [
                    h * (gz1 + gy[0]), g * (gy[1] + 0.75 * (gz0 + gy[1] + gx2)), h * (gy[2] + gx1)
                ])

        def close(step, z, row, waiting):
            for i in range(3):
                change = jnp.concatenate(
                    [TY[z, i, l, row + 1:row + 9, :] - TY[z, i, l, row - 1:row + 7, :] for l in range(L)],
                    axis=1,
                )
                store(step, i, z, row, waiting[i] + change)

        def held(step, i, z, row):
            if step:
                return moved_ref[i, z, row - TOP:row - TOP + 8, :]
            return take(1, i, z + 2, row, L)

        def strip(step, z, row, with_damage):
            wide = L + 1
            now = [take(step, f, z + 2, row, wide) for f in range(3)]
            gz = [slope_z(step, f, z, row, wide) for f in range(3)]
            gy = [slope_y(step, f, z, row, wide) for f in range(3)]
            gx = [along_x(v, wide) for v in now]
            g = gain(step, z, row, wide)
            h = 0.5 * g
            lam = 0.75 * (gz[0] + gy[1] + gx[2])
            a01 = (gz[1] + gy[0])[:, 0:C]
            a02 = gz[2] + gx[0]
            a12 = gy[2] + gx[1]
            t01, t02, t12 = h[:, 0:C] * a01, h * a02, h * a12
            put_y(z, row, [t01, (g * (gy[1] + lam))[:, 0:C], t12[:, 0:C]])
            at = slice(row - TOP, row - TOP + 8)
            TZ[z + 1, 0, at] = (g * (gz[0] + lam))[:, 0:C]
            TZ[z + 1, 1, at] = t01
            TZ[z + 1, 2, at] = t02[:, 0:C]
            if with_damage:
                hurt(
                    step, z, row, gz[0][:, 0:C], gy[1][:, 0:C], gx[2][:, 0:C],
                    a01, a02[:, 0:C], a12[:, 0:C],
                )
            return [
                now[i][:, 0:C] + along_x(t, L) for i, t in enumerate((t02, t12, g * (gx[2] + lam)))
            ]

        def force_mid(step, z, with_damage):
            for row in core_rows[1:-1]:
                for i, value in enumerate(strip(step, z, row, with_damage)):
                    store(step, i, z, row, value)

        def force_rim(step, z, with_damage):
            outer_rows(step, z)
            first = strip(step, z, core_rows[0], with_damage)
            last = strip(step, z, core_rows[-1], with_damage)
            close(step, z, core_rows[0], first)
            for row in core_rows[1:-1]:
                close(step, z, row, [held(step, i, z, row) for i in range(3)])
            close(step, z, core_rows[-1], last)

        def force(step, z):
            outer_rows(step, z)
            waiting = None
            for row in core_rows:
                ready = strip(step, z, row, False)
                if waiting is not None:
                    close(step, z, row - 8, waiting)
                waiting = ready
            close(step, z, END - 8, waiting)

        def finish(step, z):
            for i in range(3):
                for l in range(L):
                    lanes = slice(128 * l, 128 * l + 128)
                    U[1, i, z + 2, l, body_rows, :] = U[1, i, z + 2, l, body_rows, :] + (
                        TZ[z + 2, i, :, lanes] - TZ[z, i, :, lanes]
                    )

        def finish_pool(z, row):
            means = []
            for i in range(3):
                value = moved_ref[i, z] + (TZ[z + 2, i] - TZ[z, i])
                moved_ref[i, z] = value
                folded = value[:, 0:128]
                for cut in range(128, C, 128):
                    folded = folded + value[:, cut:cut + 128]
                means.append(jnp.sum(folded, axis=1, keepdims=True) * (1.0 / C))
            pooled_t[row:row + R, :] = jnp.where(
                lane_r == 0, means[0], jnp.where(lane_r == 1, means[1], means[2])
            )

        def pooled(rows_here):
            value = pooled_t[0:rows_here, :].T[0:8].astype(jnp.bfloat16)
            return jnp.concatenate([value, value], axis=1)

        settle(2 * 3 * 2 * L * R // 8, in_sem.at[0])
        with scope("barrier"):
            pl.semaphore_wait(barrier, met)
        send(0, "zu")
        pack_corners(0)
        send(0, "zx", "zy")
        crack_load.wait()

        def label(z, carry):
            for l in range(L):
                U[0, 3, z + 2, l, body_rows, :] = DAMAGE_LEVEL * crack[
                    z, :, 128 * l:128 * l + 128
                ].astype(F32)
            return carry

        lax.fori_loop(0, Z, label, 0)
        settle(3 * (Z - 4) * L * R // 8, in_sem.at[4])
        with scope("pack"):
            pack_y(0, 0)
            send(0, "y0", "yx0", "x0")
            for item in [tough_load, *weight_loads]:
                item.start()
        for side, sign in ((0, -1), (1, 1)):
            clear((sign, 0, 0), clear_z(side))
            clear((0, sign, 0), clear_y(side))
            clear((0, 0, sign), clear_x(side))

        cell_load.wait()
        base = me[0] * Z * (R * n_pencil) + me[1] * R
        row_id = lax.broadcasted_iota(jnp.int32, (R, 512), 0) * n_comp

        def choose(part, z, row):
            start = (base + z * (R * n_pencil)) * n_comp + me[2]
            for s in range(0, sensors, 512):
                hit = row_id == cell_ref[:, s:s + 512] - start
                weight[part, row:row + R, s:s + 512] = jnp.where(hit, POINT_GAIN, 0.0).astype(
                    jnp.bfloat16
                )

        with scope("choose"):
            for k, z in enumerate((0, 1, Z - 2, Z - 1)):
                choose(0, z, rim + k * R)
            for z in range(2, Z - 2):
                choose(1, z, inner + (z - 2) * R)
            tough_load.wait()
        send(0, "zd", "zs")
        with scope("waitx"):
            receive(0, "x0")
        with scope("unpx"):
            loop(0, Z, lambda z: unpack_x(0, z))
        with scope("mid"):
            loop(1, Z - 1, lambda z: force_mid(0, z, True))
        with scope("waity"):
            receive(0, "y0", "yx0")
        with scope("unpy"):
            loop(0, Z, lambda z: unpack_y(0, z, 4))
            unpack_yx(0, 0)
        with scope("body"):
            loop(0, 2, lambda k: force_rim(0, 2 + k * (Z - 5), True))
            loop(0, 2, lambda k: force_rim(0, 1 + k * (Z - 3), True))
        with scope("waitza"):
            receive(0, *EDGE)
        with scope("edge"):
            unpack_zx(0)
            for z in (-1, Z):
                unpack_y(0, z, 3)
            loop(0, 2, lambda k: ends(0, k * (Z - 1)))
            loop(0, 2, lambda k: finish(0, 1 + k * (Z - 3)))
        send(1, "zs")
        with scope("body2"):
            loop(3, Z - 3, lambda z: force_rim(0, z, True))
            loop(2, Z - 2, lambda z: finish(0, z))
            loop(0, 2, lambda k: force(0, k * (Z - 1)))
            pack_y(1, 0)
            send(1, "y0", "yx0", "x0")
        with scope("waitzb"):
            receive(0, *REST)
        with scope("ends"):
            loop(0, 2, lambda k: ends(0, k * (Z + 1) - 1))
            loop(0, 2, lambda k: finish(0, k * (Z - 1)))
        pack_corners(1)
        send(1, "zu", "zx", "zy")
        with scope("damage"):
            loop(0, 2, lambda k: damage(0, k * (Z - 1)))
        send(1, "zd")
        with scope("pack2"):
            pack_y(1, 1)
            send(1, "y1", "y2", "yx1", "x1", "x2")

        with scope("waitx"):
            receive(1, "x0")
            loop(1, Z - 1, lambda z: unpack_x(1, z))
        with scope("mid"):
            loop(2, Z - 2, lambda z: force_mid(1, z, False))
        with scope("waitxe"):
            receive(1, "x1", "x2")
        with scope("mide"):
            for z in (0, Z - 1):
                unpack_x(1, z)
            loop(0, 2, lambda k: force_mid(1, 1 + k * (Z - 3), False))
        with scope("waity"):
            receive(1, "y0", "yx0")
            loop(1, Z - 1, lambda z: unpack_y(1, z, 4))
            unpack_yx(1, 0)
        with scope("rim"):
            loop(2, Z - 2, lambda z: force_rim(1, z, False))
        with scope("waitye"):
            receive(1, "y1", "y2", "yx1")
        with scope("rime"):
            for z in (0, Z - 1):
                unpack_y(1, z, 4)
            unpack_yx(1, 1)
            loop(0, 2, lambda k: force_rim(1, 1 + k * (Z - 3), False))
        with scope("pooli"):
            for z in range(2, Z - 2):
                finish_pool(z, (z - 2) * R)
        with scope("doti"):
            settle(Z * R * sensors * 2 // 4096, in_sem.at[5])
            lhs = pooled(inner)
            for cut in range(0, sensors, 256):
                acc[:, cut:cut + 256] = jnp.dot(
                    lhs, weight[1, 0:2 * inner, cut:cut + 256], preferred_element_type=F32
                )
        with scope("waitz"):
            receive(1, *REST, *EDGE)
        with scope("edge"):
            unpack_zx(1)
            for z in (-1, Z):
                unpack_y(1, z, 3)
            loop(0, 2, lambda k: force(1, k * (Z - 1)))
            loop(0, 2, lambda k: ends(1, k * (Z + 1) - 1))
        with scope("poole"):
            for k, z in enumerate((0, 1, Z - 2, Z - 1)):
                finish_pool(z, k * R)

        def spread(stop, function):
            if stop <= 16:
                for k in range(stop):
                    function(k)
            else:
                loop(0, stop, function)

        def owner(q):
            return {"slab": first_slab + q // n_pencil, "pencil": q % n_pencil, "comp": n_comp - 1}

        def owned_by(q):
            return jnp.logical_and(mine == q, me[2] == n_comp - 1)

        def scatter(q):
            return pltpu.make_async_remote_copy(
                src_ref=partial.at[q], dst_ref=RB.at[flat],
                send_sem=send_sem.at[1], recv_sem=recv_sem.at[8],
                device_id=owner(q), device_id_type=MESH,
            )

        def landed(ref, sem):
            pltpu.make_async_copy(ref, ref, sem).wait()

        def gather(q, k):
            return pltpu.make_async_remote_copy(
                src_ref=GB.at[q], dst_ref=GB.at[q],
                send_sem=send_sem.at[2], recv_sem=recv_sem.at[9],
                device_id=device(k), device_id_type=MESH,
            )

        def unless(same, function):
            @pl.when(jnp.logical_not(same))
            def _():
                function()

        mine = (me[0] - first_slab) * n_pencil + me[1]
        owning = jnp.logical_and(
            me[2] == n_comp - 1, jnp.logical_and(mine >= 0, mine < owners)
        )
        with scope("dot"):
            lhs = pooled(rim)
            for cut in range(0, sensors, 256):
                value = acc[:, cut:cut + 256] + jnp.dot(
                    lhs, weight[0, 0:2 * rim, cut:cut + 256], preferred_element_type=F32
                )
                for low in (0, 128):
                    for c in range(3):
                        partial[(cut + low) // piece, c, (cut + low) % piece // 128] = (
                            value[c, low:low + 128]
                        )
        with scope("rssend"):
            for q in range(owners):
                unless(owned_by(q), lambda: scatter(q).start())

        with scope("damage"):
            loop(0, Z, lambda z: damage(1, z))

        @pl.when(owning)
        def _():
            with scope("waitrs"):
                landed(RB.at[0:count - 1], recv_sem.at[8])
            RB[flat] = partial[mine]
            if count <= 16:
                total = RB[0]
                for k in range(1, count):
                    total = total + RB[k]
            else:
                total = lax.fori_loop(1, count, lambda k, t: t + RB[k], RB[0])
            GB[mine] = total
            spread(count, lambda k: unless(flat == k, lambda: gather(mine, k).start()))

        with scope("waitag"):
            @pl.when(owning)
            def _():
                if owners > 1:
                    landed(GB.at[0:owners - 1], recv_sem.at[9])

            @pl.when(jnp.logical_not(owning))
            def _():
                landed(GB.at[0:owners], recv_sem.at[9])

        for q in range(owners):
            for c in range(3):
                for k in range(strips):
                    low = q * piece + 128 * k
                    read_ref[c, low:low + 128] = GB[q, c, k]
        with scope("sends"):
            settle_messages((0, 1), lambda t: SENT[t], send_sem.at[0])

            @pl.when(owning)
            def _():
                if owners > 1:
                    landed(partial.at[0:owners - 1], send_sem.at[1])
                landed(RB.at[0:count - 1], send_sem.at[2])

            @pl.when(jnp.logical_not(owning))
            def _():
                landed(partial.at[0:owners], send_sem.at[1])

    return kernel


def emit(moved_ref, damage_ref, read_ref, moved_hbm, damage_hbm, read_hbm, sem):
    copies = [
        pltpu.make_async_copy(moved_ref, moved_hbm, sem.at[0]),
        pltpu.make_async_copy(damage_ref, damage_hbm, sem.at[1]),
        pltpu.make_async_copy(read_ref, read_hbm, sem.at[2]),
    ]
    for copy in copies:
        copy.start()
    for copy in copies:
        copy.wait()


def solution(mesh):
    sizes = tuple(mesh.shape[a] for a in AXES)
    n_slab = sizes[0]
    count = sizes[0] * sizes[1] * sizes[2]

    def local(u_start, toughness, crack_label, obs_weight, sensor_cell):
        Z, R, C = toughness.shape
        S = sensor_cell.shape[0]
        first_slab = max(n_slab // 2 - 1, 0)
        owners = min(2, n_slab) * sizes[1]
        while S % (owners * 256):
            owners -= 1
        piece = S // owners
        rim, inner = 4 * R, (Z - 4) * R
        most = max(
            Z * R * S * 2 // 4096,
            sum(group_tiles(t, SENT[t], (2, 2, 2), Z, R, C // 128) for t in range(2)),
        )
        any_spec = pl.BlockSpec(memory_space=pltpu.HBM)
        vmem_spec = pl.BlockSpec(memory_space=pltpu.VMEM)
        dma = pltpu.SemaphoreType.DMA
        shapes = (
            jax.ShapeDtypeStruct((3, Z, R, C), F32),
            jax.ShapeDtypeStruct((Z, R, C), F32),
            jax.ShapeDtypeStruct((3, S), F32),
        )
        outs = pl.pallas_call(
            make_kernel(Z, R, C, S, sizes, first_slab, owners),
            out_shape=shapes,
            in_specs=[any_spec] * 5,
            out_specs=[vmem_spec] * 3,
            scratch_shapes=[
                pltpu.VMEM((2, 4, Z + 4, C // 128 + 1, R + 32, 128), F32),
                pltpu.VMEM((2, 2, 4, Z, R, 128), F32),
                pltpu.VMEM((2, 2, 2, 8, 128), F32),
                pltpu.VMEM((2, 2, 2, 8, 128), F32),
                pltpu.VMEM((2, 2, Z + 2, 8, C), F32),
                pltpu.VMEM((2, 2, Z, 8, C), F32),
                pltpu.VMEM((2, 2, 2, 8, C), F32),
                pltpu.VMEM((2, 2, 2, 2, 8, 128), F32),
                pltpu.VMEM((2, 2, 2, 2, 8, 128), F32),
                pltpu.VMEM((Z + 2, 3, R, C), F32),
                pltpu.VMEM((Z, 3, C // 128, R + 32, 128), F32),
                pltpu.VMEM((most, 8, 128), F32),
                pltpu.VMEM((Z, R, C), F32),
                pltpu.VMEM((Z, R, C), jnp.int32),
                pltpu.VMEM((2, 2 * max(rim, inner), S), jnp.bfloat16),
                pltpu.VMEM((1, S), jnp.int32),
                pltpu.VMEM((max(rim, inner), 128), F32),
                pltpu.VMEM((8, S), F32),
                pltpu.VMEM((owners, 3, piece // 128, 128), F32),
                pltpu.VMEM((count, 3, piece // 128, 128), F32),
                pltpu.VMEM((owners, 3, piece // 128, 128), F32),
                dma((6,)),
                dma((3,)),
                dma((11,)),
            ],
            compiler_params=pltpu.CompilerParams(
                collective_id=0, has_side_effects=True, vmem_limit_bytes=40 * 1024 * 1024
            ),
            name="fracture",
        )(
            *[
                pltpu.with_memory_space_constraint(x, pltpu.HBM)
                for x in (
                    u_start, toughness, crack_label, obs_weight.reshape(Z * R, S),
                    sensor_cell.reshape(1, S),
                )
            ],
        )
        return pl.pallas_call(
            emit,
            out_shape=shapes,
            in_specs=[vmem_spec] * 3,
            out_specs=[any_spec] * 3,
            scratch_shapes=[dma((3,))],
            name="emit",
        )(*[pltpu.with_memory_space_constraint(x, pltpu.VMEM) for x in outs])

    return jax.shard_map(
        local,
        mesh=mesh,
        in_specs=(
            P(None, ("groups", "slab"), "pencil", "comp"),
            P(("groups", "slab"), "pencil", "comp"),
            P(("groups", "slab"), "pencil", "comp"),
            P("slab", "pencil", "comp", None),
            P(),
        ),
        out_specs=(
            P(None, ("groups", "slab"), "pencil", "comp"),
            P(("groups", "slab"), "pencil", "comp"),
            P(None, "groups"),
        ),
        check_vma=False,
    )
```

```python
import itertools

import jax
import jax.numpy as jnp
import numpy as np
from jax import lax
from jax.experimental import pallas as pl
from jax.experimental.pallas import tpu as pltpu
from jax.sharding import PartitionSpec as P

RESIDUAL_STIFF = 0.001
TIME_DISP = 0.15
TIME_DAMAGE = 0.08
DAMAGE_LEVEL = 0.45
POINT_GAIN = 8.0
AXES = ("slab", "pencil", "comp")
MESH = pl.DeviceIdType.MESH
F32 = jnp.float32


def third_angle_poly():
    nodes = 0.5 + 0.5 * np.cos(np.pi * (np.arange(200) + 0.5) / 200)
    fit = np.polynomial.chebyshev.Chebyshev.fit(
        nodes, np.cos(np.arccos(nodes) / 3.0), 8, domain=[0.0, 1.0]
    )
    return [float(c) for c in fit.convert(kind=np.polynomial.Polynomial).coef]


POLY = third_angle_poly()

DIRECTIONS = [
    d for d in itertools.product((-1, 0, 1), repeat=3) if 1 <= sum(map(abs, d)) <= 2
]
ALONG_Z = [d for d in DIRECTIONS if d[0] and not d[1] and not d[2]]
ALONG_Y = [d for d in DIRECTIONS if d[1] and not d[0] and not d[2]]
ALONG_X = [d for d in DIRECTIONS if d[2] and not d[0] and not d[1]]
DIAG_ZY = [d for d in DIRECTIONS if d[0] and d[1]]
DIAG_ZX = [d for d in DIRECTIONS if d[0] and d[2]]
DIAG_YX = [d for d in DIRECTIONS if d[1] and d[2]]
KINDS = (
    [("zu", d) for d in ALONG_Z] + [("zy", d) for d in DIAG_ZY] + [("zx", d) for d in DIAG_ZX]
    + [("zd", d) for d in ALONG_Z] + [("zs", d) for d in ALONG_Z]
    + [(k, d) for k in ("y0", "y1", "y2") for d in ALONG_Y]
    + [(k, d) for k in ("yx0", "yx1") for d in DIAG_YX]
    + [(k, d) for k in ("x0", "x1", "x2") for d in ALONG_X]
)
EDGE = ("zu", "zy", "zx")
REST = ("zd", "zs")


def energy_of(g0, g1, g2, a01, a02, a12):
    trace = g0 + g1 + g2
    mean = trace * (1.0 / 3.0)
    d0, d1, d2 = g0 - mean, g1 - mean, g2 - mean
    q01, q02, q12 = a01 * a01, a02 * a02, a12 * a12
    d01 = d0 * d1
    p2 = (d0 * d0 + d1 * d1 + d01) * (1.0 / 3.0) + (q01 + q02 + q12) * (1.0 / 12.0)
    inv = lax.rsqrt(jnp.maximum(p2, 1e-36))
    p = p2 * inv
    det = d01 * d2 + 0.25 * (a01 * a02 * a12 - d0 * q12 - d1 * q02 - d2 * q01)
    half_det = ((det * inv) * inv) * (0.5 * inv)
    r = jnp.minimum(jnp.abs(half_det), 1.0)
    c = jnp.full_like(r, POLY[-1])
    for coefficient in POLY[-2::-1]:
        c = c * r + coefficient
    tc = p * c
    t = jnp.where(half_det < 0.0, -tc, tc)
    s2 = jnp.maximum(1.0 - c * c, 0.0)
    delta = p * (s2 * lax.rsqrt(jnp.maximum(s2, 1e-30))) * float(np.sqrt(3.0))
    f1 = jnp.maximum(mean + 2.0 * t, 0.0)
    f2 = jnp.maximum(mean - t + delta, 0.0)
    f3 = jnp.maximum(mean - t - delta, 0.0)
    ft = jnp.maximum(trace, 0.0)
    return 0.75 * ft * ft + f1 * f1 + f2 * f2 + f3 * f3


def message_tiles(kind, step, Z, R, L):
    if kind in ("zu", "zs"):
        return 3 * L * R // 8
    if kind == "zd":
        return L * R // 8
    if kind == "zx":
        return 1
    if kind == "zy":
        return L
    if kind[:2] == "yx":
        return 1
    planes = 1 if kind[1] != "0" else Z - 2 if step else Z
    return planes * L if kind[0] == "y" else planes * 4 * R // 8


SENT = [
    ("zu", "zx", "zy", "zd", "zs", "y0", "yx0", "x0"),
    ("zu", "zx", "zy", "zd", "zs", "y0", "yx0", "x0", "y1", "y2", "yx1", "x1", "x2"),
]


def group_tiles(step, kinds, met, Z, R, L):
    total = 0
    for kind in kinds:
        number = message_tiles(kind, step, Z, R, L)
        axes = [a for a, name in enumerate("zyx") if name in kind[:2]]
        for a in axes if kind[:2] in ("zx", "zy", "yx") else axes[:1]:
            number *= met[a]
        total += number
    return total


def make_kernel(planes, rows, columns, sensors, sizes, first_slab, owners):
    n_slab, n_pencil, n_comp = sizes
    count = n_slab * n_pencil * n_comp
    Z, R, C = planes, rows, columns
    piece = sensors // owners
    strips = piece // 128
    L = C // 128
    TOP = 16
    END = TOP + R
    body_rows = slice(TOP, END)
    rim = 4 * R
    spans = {
        0: {"0": (0, Z)},
        1: {"0": (1, Z - 1), "1": (0, 1), "2": (Z - 1, Z)},
    }
    groups = {0: [range(Z)], 1: [range(1, Z - 1), [0, Z - 1]]}
    near = n_slab <= 4 and n_pencil <= 2 and n_comp <= 2

    def scope(name):
        return jax.named_scope(name)

    def kernel(u_hbm, tough_hbm, crack_hbm, weight_hbm, cell_hbm,
               moved_ref, damage_ref, read_ref,
               U, XR, XS, XC, YR, YP, YZ, YX, YXR, TZ, TY, W, tough, crack, weight, cell_ref, pooled_t, acc,
               partial, RB, GB,
               in_sem, send_sem, recv_sem):
        me = [lax.axis_index(a) for a in AXES]
        flat = (me[0] * n_pencil + me[1]) * n_comp + me[2]

        def device(index):
            return {
                "slab": index // (n_pencil * n_comp),
                "pencil": (index // n_comp) % n_pencil,
                "comp": index % n_comp,
            }

        def u_load(k, low, high):
            return [
                pltpu.make_async_copy(
                    u_hbm.at[:, low:high, :, 128 * l:128 * l + 128],
                    U.at[0, 0:3, low + 2:high + 2, l, body_rows, :],
                    in_sem.at[4 if k == 2 else 0],
                )
                for l in range(L)
            ]

        edge_loads = u_load(0, 0, 2) + u_load(1, Z - 2, Z)
        inner_loads = u_load(2, 2, Z - 2)
        crack_load = pltpu.make_async_copy(crack_hbm, crack, in_sem.at[1])
        tough_load = pltpu.make_async_copy(tough_hbm, tough, in_sem.at[2])
        cell_load = pltpu.make_async_copy(cell_hbm, cell_ref, in_sem.at[3])
        inner = Z * R - rim
        weight_loads = [
            pltpu.make_async_copy(weight_hbm.at[0:rim // 2], weight.at[0, 0:rim // 2], in_sem.at[5]),
            pltpu.make_async_copy(
                weight_hbm.at[Z * R - rim // 2:Z * R], weight.at[0, rim // 2:rim], in_sem.at[5]),
            pltpu.make_async_copy(
                weight_hbm.at[rim // 2:Z * R - rim // 2], weight.at[1, 0:inner], in_sem.at[5]),
        ]
        for item in edge_loads:
            item.start()

        barrier = pltpu.get_barrier_semaphore()

        def inside(d, sign):
            ok = None
            for m, o, n in zip(me, d, sizes):
                if o:
                    here = m + 1 < n if sign * o > 0 else m >= 1
                    ok = here if ok is None else jnp.logical_and(ok, here)
            return ok

        def feasible(d):
            return all(n > 1 for o, n in zip(d, sizes) if o)

        def neighbour(d):
            return {a: m + o for a, m, o in zip(AXES, me, d)}

        met = 0
        if near:
            for d in DIRECTIONS:
                if feasible(d):
                    @pl.when(inside(d, 1))
                    def _():
                        pl.semaphore_signal(
                            barrier, inc=1, device_id=neighbour(d), device_id_type=MESH
                        )

                    met = met + inside(d, 1).astype(jnp.int32)
        else:
            def greet(k, carry):
                pl.semaphore_signal(
                    barrier, inc=1, device_id=device((flat + k) % count), device_id_type=MESH
                )
                return carry

            lax.fori_loop(1, count, greet, 0)
            met = count - 1

        for item in [crack_load, *inner_loads, cell_load]:
            item.start()

        def clear(d, write):
            if feasible(d):
                @pl.when(jnp.logical_not(inside(d, 1)))
                def _():
                    write()
            else:
                write()

        def clear_z(up):
            def write():
                for step in range(2):
                    for z in ((Z + 2, Z + 3) if up else (0, 1)):
                        U[step, :, z, 0:L, body_rows] = jnp.zeros((4, L, R, 128), F32)
                XC[:, up] = jnp.zeros((2, 2, 8, 128), F32)
                for step in range(2):
                    for side in range(2):
                        YR[step, side, (Z + 1) * up] = jnp.zeros((8, C), F32)
            return write

        def clear_x(right):
            def write():
                def one(k, carry):
                    XR[k // (4 * Z), right, (k // Z) % 4, k % Z] = jnp.zeros((R, 128), F32)
                    return carry

                lax.fori_loop(0, 8 * Z, one, 0)
                XC[:, :, right] = jnp.zeros((2, 2, 8, 128), F32)
                YXR[:, :, right] = jnp.zeros((2, 2, 2, 8, 128), F32)
            return write

        def clear_y(up):
            def write():
                YR[:, up] = jnp.zeros((2, Z + 2, 8, C), F32)
                YXR[:, up] = jnp.zeros((2, 2, 2, 8, 128), F32)
            return write

        core_rows = range(TOP, END, 8)
        row8t = lax.broadcasted_iota(jnp.int32, (8, 128), 0)
        lane8 = lax.broadcasted_iota(jnp.int32, (8, 128), 1)
        lane_r = lax.broadcasted_iota(jnp.int32, (R, 128), 1)

        def roll(value, shift, axis):
            shift = shift % value.shape[axis]
            return pltpu.roll(value, shift, axis) if shift else value

        def loop(start, stop, function):
            def one(z, carry):
                function(z)
                return carry

            lax.fori_loop(start, stop, one, 0)

        def slot(step, kind):
            if step == 0:
                return 0 if kind in EDGE else 1 if kind in REST else 2 if kind[0] == "x" else 3
            if kind[0] == "z":
                return 4
            if kind[-1] == "0":
                return 5 if kind[0] == "x" else 6
            return 10 if kind[0] == "x" else 7

        def message(step, kind, d):
            dz, dy, dx = d
            sz, sy, sx = (dz + 1) // 2, (dy + 1) // 2, (dx + 1) // 2
            tile = L - 1 if dx > 0 else 0
            edge = Z - 1 if dz > 0 else 0
            halo = 0 if dz > 0 else Z + 1
            if kind == "zu":
                pair = (
                    U.at[step, 0:3, edge + 2, 0:L, body_rows], U.at[step, 0:3, halo + 1, 0:L, body_rows]
                )
            elif kind == "zs":
                pair = (
                    U.at[step, 0:3, Z if dz > 0 else 3, 0:L, body_rows],
                    U.at[step, 0:3, 0 if dz > 0 else Z + 3, 0:L, body_rows],
                )
            elif kind == "zd":
                pair = (U.at[step, 3, edge + 2, 0:L, body_rows], U.at[step, 3, halo + 1, 0:L, body_rows])
            elif kind == "zy":
                pair = (YZ.at[step, sy, sz], YR.at[step, 1 - sy, halo])
            elif kind == "zx":
                pair = (XS.at[step, sz, sx], XC.at[step, 1 - sz, 1 - sx])
            elif kind[:2] == "yx":
                part = int(kind[2])
                pair = (YX.at[step, sy, sx, part], YXR.at[step, 1 - sy, 1 - sx, part])
            else:
                low, high = spans[step][kind[1]]
                if kind[0] == "y":
                    pair = (YP.at[step, sy, low:high], YR.at[step, 1 - sy, low + 1:high + 1])
                else:
                    pair = (
                        U.at[step, :, low + 2:high + 2, tile, body_rows],
                        XR.at[step, 1 - sx, :, low:high],
                    )
            return pltpu.make_async_remote_copy(
                src_ref=pair[0],
                dst_ref=pair[1],
                send_sem=send_sem.at[0],
                recv_sem=recv_sem.at[slot(step, kind)],
                device_id=neighbour(d),
                device_id_type=MESH,
            )

        def each(step, kinds, sign, action):
            for name in kinds:
                for kind, d in KINDS:
                    if kind == name and feasible(d):
                        @pl.when(inside(d, sign))
                        def _():
                            action(message(step, kind, d))

        def settle(tiles, sem):
            if tiles:
                pltpu.make_async_copy(W.at[0:tiles], W.at[0:tiles], sem).wait()

        def settle_messages(steps, kinds, sem):
            for number in itertools.product(*[
                (0,) if n == 1 else (1,) if n == 2 else (1, 2) for n in sizes
            ]):
                here = None
                for m, n, k in zip(me, sizes, number):
                    if n > 2:
                        both = jnp.logical_and(m > 0, m < n - 1)
                        ok = both if k == 2 else jnp.logical_not(both)
                        here = ok if here is None else jnp.logical_and(here, ok)
                tiles = sum(group_tiles(t, kinds(t), number, Z, R, L) for t in steps)

                def wait():
                    settle(tiles, sem)

                if here is None:
                    wait()
                else:
                    pl.when(here)(wait)

        def send(step, *kinds):
            each(step, kinds, 1, lambda copy: copy.start())

        def receive(step, *kinds):
            settle_messages((step,), lambda _: kinds, recv_sem.at[slot(step, kinds[0])])

        def pack_plane(step, z, save):
            for side, firsts in (
                (0, [TOP - 2 * f for f in range(4)]),
                (1, [END - 2 - 2 * f for f in range(3)] + [END - 7]),
            ):
                for l in range(L):
                    rows = [U[step, f, z + 2, l, at:at + 8, :] for f, at in enumerate(firsts)]
                    save(side, l, jnp.where(
                        row8t < 2, rows[0],
                        jnp.where(row8t < 4, rows[1], jnp.where(row8t < 6, rows[2], rows[3])),
                    ))

        def pack_y(step, part):
            for z in groups[step][part]:
                def save(side, l, value):
                    YP[step, side, z, :, 128 * l:128 * l + 128] = value

                pack_plane(step, z, save)
            for side in range(2):
                for sx in range(2):
                    tile = jnp.zeros((8, 128), F32)
                    for z in groups[step][part]:
                        value = YP[step, side, z, :, (C - 128) * sx:(C - 128) * sx + 128]
                        tile = jnp.where(lane8 == z, roll(value, z + sx, 1), tile)
                    YX[step, side, sx, part] = tile

        def pack_corners(step):
            for sz, z in ((0, 0), (1, Z - 1)):
                for sx in range(2):
                    tile = jnp.zeros((8, 128), F32)
                    for k, row in enumerate(core_rows):
                        for f in range(3):
                            value = U[step, f, z + 2, (L - 1) * sx, row:row + 8, :]
                            lane = 3 * k + f
                            tile = jnp.where(lane8 == lane, roll(value, lane + sx, 1), tile)
                    XS[step, sz, sx] = tile

                def save(side, l, value):
                    YZ[step, side, sz, :, 128 * l:128 * l + 128] = value

                pack_plane(step, z, save)

        def unpack_x(step, z):
            for f in range(4):
                U[step, f, z + 2, L, body_rows, :] = jnp.where(
                    lane_r < 64, XR[step, 1, f, z], XR[step, 0, f, z]
                )

        def unpack_zx(step):
            for sz, z in ((0, -1), (1, Z)):
                right, left = XC[step, sz, 1], XC[step, sz, 0]
                for k, row in enumerate(core_rows):
                    for f in range(3):
                        lane = 3 * k + f
                        U[step, f, z + 2, L, row:row + 8, :] = jnp.where(
                            lane8 < 64, roll(right, -lane, 1), roll(left, 127 - lane, 1)
                        )

        def put_rows(step, z, l, low, high, fields):
            for f in range(fields):
                if f < 3:
                    U[step, f, z + 2, l, TOP - 2:TOP, :] = low[2 * f:2 * f + 2]
                    U[step, f, z + 2, l, END:END + 2, :] = high[2 * f:2 * f + 2]
                else:
                    U[step, f, z + 2, l, TOP - 1:TOP, :] = low[6:7]
                    U[step, f, z + 2, l, END:END + 1, :] = high[6:7]

        def unpack_y(step, z, fields):
            for l in range(L):
                low, high = [YR[step, side, z + 1, :, 128 * l:128 * l + 128] for side in range(2)]
                put_rows(step, z, l, low, high, fields)

        def unpack_yx(step, part):
            for z in groups[step][part]:
                low, high = [
                    jnp.where(
                        lane8 < 64, roll(YXR[step, sy, 1, part], -z, 1),
                        roll(YXR[step, sy, 0, part], 127 - z, 1),
                    )
                    for sy in range(2)
                ]
                put_rows(step, z, L, low, high, 3)

        def take(step, f, z, row, tiles):
            parts = [U[step, f, z, l, row:row + 8, :] for l in range(tiles)]
            return jnp.concatenate(parts, axis=1)

        def slope_z(step, f, z, row, tiles):
            return take(step, f, z + 3, row, tiles) - take(step, f, z + 1, row, tiles)

        def slope_y(step, f, z, row, tiles):
            return take(step, f, z + 2, row + 1, tiles) - take(step, f, z + 2, row - 1, tiles)

        def beside(value, tiles):
            parts = [value[:, 128 * l:128 * l + 128] for l in range(L + 1)]
            after, before = [], []
            for l in range(tiles):
                after.append(roll(jnp.where(lane8 == 0, parts[(l + 1) % (L + 1)], parts[l]), -1, 1))
                before.append(roll(jnp.where(lane8 == 127, parts[l - 1], parts[l]), 1, 1))
            return jnp.concatenate(after, axis=1), jnp.concatenate(before, axis=1)

        def along_x(value, tiles):
            after, before = beside(value, tiles)
            return after - before

        def slope_x(step, f, z, row):
            return along_x(take(step, f, z + 2, row, L + 1), L)

        def gain(step, z, row, tiles):
            keep = 1.0 - take(step, 3, z + 2, row, tiles)
            return (0.5 * TIME_DISP) * (keep * keep + RESIDUAL_STIFF)

        def store(step, f, z, row, value):
            if step == 0:
                for l in range(L):
                    U[1, f, z + 2, l, row:row + 8, :] = value[:, 128 * l:128 * l + 128]
            elif f < 3:
                moved_ref[f, z, row - TOP:row - TOP + 8, :] = value
            else:
                damage_ref[z, row - TOP:row - TOP + 8, :] = value

        def ends(step, z):
            for row in core_rows:
                gz = [slope_z(step, f, z, row, L) for f in range(3)]
                gy0, gy1 = slope_y(step, 0, z, row, L), slope_y(step, 1, z, row, L)
                gx0, gx2 = slope_x(step, 0, z, row), slope_x(step, 2, z, row)
                g = gain(step, z, row, L)
                h = 0.5 * g
                at = slice(row - TOP, row - TOP + 8)
                TZ[z + 1, 0, at] = g * (gz[0] + 0.75 * (gz[0] + gy1 + gx2))
                TZ[z + 1, 1, at] = h * (gz[1] + gy0)
                TZ[z + 1, 2, at] = h * (gz[2] + gx0)

        def hurt(step, z, row, gz0, gy1, gx2, a01, a02, a12):
            energy = energy_of(gz0, gy1, gx2, a01, a02, a12)
            dx = take(step, 3, z + 2, row, L + 1)
            dc = dx[:, 0:C]
            after, before = beside(dx, L)
            lap = (
                take(step, 3, z + 3, row, L) + take(step, 3, z + 1, row, L)
                + take(step, 3, z + 2, row + 1, L) + take(step, 3, z + 2, row - 1, L)
                + (after + before)
                - 7.0 * dc
            )
            store(step, 3, z, row, dc + TIME_DAMAGE * (
                0.5 * (1.0 - dc) * energy + tough[z, row - TOP:row - TOP + 8, :] * lap
            ))

        def damage(step, z):
            for row in core_rows:
                gz = [slope_z(step, f, z, row, L) for f in range(3)]
                gy = [slope_y(step, f, z, row, L) for f in range(3)]
                gx = [slope_x(step, f, z, row) for f in range(3)]
                hurt(
                    step, z, row, gz[0], gy[1], gx[2],
                    gz[1] + gy[0], gz[2] + gx[0], gy[2] + gx[1],
                )

        def put_y(z, row, values):
            for i in range(3):
                for l in range(L):
                    TY[z, i, l, row:row + 8, :] = values[i][:, 128 * l:128 * l + 128]

        def outer_rows(step, z, flat=False):
            for row in (TOP - 8, END):
                gy = [slope_y(step, f, z, row, L) for f in range(3)]
                gx1, gx2 = [slope_x(step, f, z, row) for f in (1, 2)]
                g = gain(step, z, row, L)
                h = 0.5 * g
                a01, trace = gy[0], gy[1] + gx2
                if not flat:
                    a01 = a01 + slope_z(step, 1, z, row, L)
                    trace = trace + slope_z(step, 0, z, row, L)
                put_y(z, row, [h * a01, g * (gy[1] + 0.75 * trace), h * (gy[2] + gx1)])

        def close(step, z, row, waiting):
            for i in range(3):
                change = jnp.concatenate(
                    [TY[z, i, l, row + 1:row + 9, :] - TY[z, i, l, row - 1:row + 7, :] for l in range(L)],
                    axis=1,
                )
                store(step, i, z, row, waiting[i] + change)

        def held(step, i, z, row):
            if step:
                return moved_ref[i, z, row - TOP:row - TOP + 8, :]
            return take(1, i, z + 2, row, L)

        def strip(step, z, row, with_damage, flat=False):
            wide = L + 1
            now = [take(step, f, z + 2, row, wide) for f in range(3)]
            gy = [slope_y(step, f, z, row, wide) for f in range(3)]
            gx = [along_x(v, wide) for v in now]
            g = gain(step, z, row, wide)
            h = 0.5 * g
            trace = gy[1] + gx[2]
            a01 = gy[0][:, 0:C]
            a02 = gx[0]
            if not flat:
                gz = [slope_z(step, f, z, row, wide) for f in range(3)]
                trace = trace + gz[0]
                a01 = a01 + gz[1][:, 0:C]
                a02 = a02 + gz[2]
            lam = 0.75 * trace
            a12 = gy[2] + gx[1]
            t01, t02, t12 = h[:, 0:C] * a01, h * a02, h * a12
            put_y(z, row, [t01, (g * (gy[1] + lam))[:, 0:C], t12[:, 0:C]])
            at = slice(row - TOP, row - TOP + 8)
            TZ[z + 1, 0, at] = (g * (lam if flat else gz[0] + lam))[:, 0:C]
            TZ[z + 1, 1, at] = t01
            TZ[z + 1, 2, at] = t02[:, 0:C]
            if with_damage:
                hurt(
                    step, z, row, gz[0][:, 0:C], gy[1][:, 0:C], gx[2][:, 0:C],
                    a01, a02[:, 0:C], a12[:, 0:C],
                )
            return [
                now[i][:, 0:C] + along_x(t, L) for i, t in enumerate((t02, t12, g * (gx[2] + lam)))
            ]

        def force_mid(step, z, with_damage, flat=False):
            for row in core_rows[1:-1]:
                for i, value in enumerate(strip(step, z, row, with_damage, flat)):
                    store(step, i, z, row, value)

        def force_rim(step, z, with_damage, flat=False):
            outer_rows(step, z, flat)
            first = strip(step, z, core_rows[0], with_damage, flat)
            last = strip(step, z, core_rows[-1], with_damage, flat)
            close(step, z, core_rows[0], first)
            for row in core_rows[1:-1]:
                close(step, z, row, [held(step, i, z, row) for i in range(3)])
            close(step, z, core_rows[-1], last)

        def force(step, z):
            outer_rows(step, z)
            waiting = None
            for row in core_rows:
                ready = strip(step, z, row, False)
                if waiting is not None:
                    close(step, z, row - 8, waiting)
                waiting = ready
            close(step, z, END - 8, waiting)

        def add_z(z):
            def put(row, first, second):
                for l in range(L):
                    lanes = slice(128 * l, 128 * l + 128)
                    TY[z, 0, l, row:row + 8, :] = first[:, lanes]
                    TY[z, 1, l, row:row + 8, :] = second[:, lanes]

            def close_two(row, waiting):
                at = slice(row - TOP, row - TOP + 8)
                for i in range(3):
                    value = moved_ref[i, z, at, :]
                    if i != 1:
                        value = value + waiting[i // 2]
                    if i < 2:
                        value = value + jnp.concatenate(
                            [
                                TY[z, i, l, row + 1:row + 9, :] - TY[z, i, l, row - 1:row + 7, :]
                                for l in range(L)
                            ],
                            axis=1,
                        )
                    moved_ref[i, z, at, :] = value

            for row in (TOP - 8, END):
                g = gain(1, z, row, L)
                put(
                    row, (0.5 * g) * slope_z(1, 1, z, row, L),
                    (0.75 * g) * slope_z(1, 0, z, row, L),
                )
            waiting = None
            for row in core_rows:
                at = slice(row - TOP, row - TOP + 8)
                g = gain(1, z, row, L + 1)
                h = 0.5 * g
                p = g * slope_z(1, 0, z, row, L + 1)
                q1 = h[:, 0:C] * slope_z(1, 1, z, row, L)
                q2 = h * slope_z(1, 2, z, row, L + 1)
                lam = 0.75 * p
                put(row, q1, lam[:, 0:C])
                TZ[z + 1, 0, at] = TZ[z + 1, 0, at] + (p + lam)[:, 0:C]
                TZ[z + 1, 1, at] = TZ[z + 1, 1, at] + q1
                TZ[z + 1, 2, at] = TZ[z + 1, 2, at] + q2[:, 0:C]
                ready = [along_x(q2, L), along_x(lam, L)]
                if waiting is not None:
                    close_two(row - 8, waiting)
                waiting = ready
            close_two(END - 8, waiting)

        def finish(step, z):
            for i in range(3):
                for l in range(L):
                    lanes = slice(128 * l, 128 * l + 128)
                    U[1, i, z + 2, l, body_rows, :] = U[1, i, z + 2, l, body_rows, :] + (
                        TZ[z + 2, i, :, lanes] - TZ[z, i, :, lanes]
                    )

        def finish_pool(z, row):
            means = []
            for i in range(3):
                value = moved_ref[i, z] + (TZ[z + 2, i] - TZ[z, i])
                moved_ref[i, z] = value
                folded = value[:, 0:128]
                for cut in range(128, C, 128):
                    folded = folded + value[:, cut:cut + 128]
                means.append(jnp.sum(folded, axis=1, keepdims=True) * (1.0 / C))
            pooled_t[row:row + R, :] = jnp.where(
                lane_r == 0, means[0], jnp.where(lane_r == 1, means[1], means[2])
            )

        def pooled(rows_here):
            value = pooled_t[0:rows_here, :].T[0:8].astype(jnp.bfloat16)
            return jnp.concatenate([value, value], axis=1)

        settle(2 * 3 * 2 * L * R // 8, in_sem.at[0])
        with scope("barrier"):
            pl.semaphore_wait(barrier, met)
        send(0, "zu")
        crack_load.wait()

        def label(z, carry):
            for l in range(L):
                U[0, 3, z + 2, l, body_rows, :] = DAMAGE_LEVEL * crack[
                    z, :, 128 * l:128 * l + 128
                ].astype(F32)
            return carry

        lax.fori_loop(0, Z, label, 0)
        settle(3 * (Z - 4) * L * R // 8, in_sem.at[4])
        with scope("pack"):
            pack_y(0, 0)
            send(0, "y0", "yx0", "x0")
            pack_corners(0)
            send(0, "zx", "zy")
            for item in [tough_load, *weight_loads]:
                item.start()
        for side, sign in ((0, -1), (1, 1)):
            clear((sign, 0, 0), clear_z(side))
            clear((0, sign, 0), clear_y(side))
            clear((0, 0, sign), clear_x(side))

        cell_load.wait()
        base = me[0] * Z * (R * n_pencil) + me[1] * R
        row_id = lax.broadcasted_iota(jnp.int32, (R, 512), 0) * n_comp

        def choose(part, z, row):
            start = (base + z * (R * n_pencil)) * n_comp + me[2]
            for s in range(0, sensors, 512):
                hit = row_id == cell_ref[:, s:s + 512] - start
                weight[part, row:row + R, s:s + 512] = jnp.where(hit, POINT_GAIN, 0.0).astype(
                    jnp.bfloat16
                )

        with scope("choose"):
            for k, z in enumerate((0, 1, Z - 2, Z - 1)):
                choose(0, z, rim + k * R)
            for z in range(2, Z - 2):
                choose(1, z, inner + (z - 2) * R)
            tough_load.wait()
        send(0, "zd", "zs")
        with scope("waitx"):
            receive(0, "x0")
        with scope("unpx"):
            loop(0, Z, lambda z: unpack_x(0, z))
        with scope("mid"):
            loop(1, Z - 1, lambda z: force_mid(0, z, True))
        with scope("waity"):
            receive(0, "y0", "yx0")
        with scope("unpy"):
            loop(0, Z, lambda z: unpack_y(0, z, 4))
            unpack_yx(0, 0)
        with scope("body"):
            loop(0, 2, lambda k: force_rim(0, 2 + k * (Z - 5), True))
            loop(0, 2, lambda k: force_rim(0, 1 + k * (Z - 3), True))
        with scope("waitza"):
            receive(0, *EDGE)
        with scope("edge"):
            loop(0, 2, lambda k: ends(0, k * (Z - 1)))
            loop(0, 2, lambda k: finish(0, 1 + k * (Z - 3)))
        send(1, "zs")
        unpack_zx(0)
        for z in (-1, Z):
            unpack_y(0, z, 3)
        with scope("body2"):
            loop(3, Z - 3, lambda z: force_rim(0, z, True))
            loop(2, Z - 2, lambda z: finish(0, z))
            loop(0, 2, lambda k: force(0, k * (Z - 1)))
            pack_y(1, 0)
            send(1, "y0", "yx0", "x0")
        with scope("waitzb"):
            receive(0, *REST)
        with scope("ends"):
            loop(0, 2, lambda k: ends(0, k * (Z + 1) - 1))
            loop(0, 2, lambda k: finish(0, k * (Z - 1)))
        pack_corners(1)
        send(1, "zu", "zx", "zy")
        with scope("damage"):
            loop(0, 2, lambda k: damage(0, k * (Z - 1)))
        send(1, "zd")
        with scope("pack2"):
            pack_y(1, 1)
            send(1, "y1", "y2", "yx1", "x1", "x2")

        with scope("waitx"):
            receive(1, "x0")
            loop(1, Z - 1, lambda z: unpack_x(1, z))
        with scope("mid"):
            loop(2, Z - 2, lambda z: force_mid(1, z, False))
        with scope("waitxe"):
            receive(1, "x1", "x2")
        with scope("mide"):
            for z in (0, Z - 1):
                unpack_x(1, z)
            loop(0, 2, lambda k: force_mid(1, 1 + k * (Z - 3), False))
            loop(0, 2, lambda k: force_mid(1, k * (Z - 1), False, True))
        with scope("waity"):
            receive(1, "y0", "yx0")
            loop(1, Z - 1, lambda z: unpack_y(1, z, 4))
            unpack_yx(1, 0)
        with scope("rim"):
            loop(2, Z - 2, lambda z: force_rim(1, z, False))
        with scope("waitye"):
            receive(1, "y1", "y2", "yx1")
        with scope("rime"):
            for z in (0, Z - 1):
                unpack_y(1, z, 4)
            unpack_yx(1, 1)
            loop(0, 2, lambda k: force_rim(1, 1 + k * (Z - 3), False))
        with scope("pooli"):
            for z in range(2, Z - 2):
                finish_pool(z, (z - 2) * R)
        with scope("doti"):
            settle(Z * R * sensors * 2 // 4096, in_sem.at[5])
            lhs = pooled(inner)
            for cut in range(0, sensors, 256):
                acc[:, cut:cut + 256] = jnp.dot(
                    lhs, weight[1, 0:2 * inner, cut:cut + 256], preferred_element_type=F32
                )
        with scope("flat"):
            loop(0, 2, lambda k: force_rim(1, k * (Z - 1), False, True))
        with scope("waitz"):
            receive(1, *REST, *EDGE)
        with scope("edge"):
            unpack_zx(1)
            for z in (-1, Z):
                unpack_y(1, z, 3)
            for k in range(2):
                ends(1, k * (Z + 1) - 1)
                add_z(k * (Z - 1))
        with scope("poole"):
            for k, z in enumerate((0, 1, Z - 2, Z - 1)):
                finish_pool(z, k * R)

        def spread(stop, function):
            if stop <= 16:
                for k in range(stop):
                    function(k)
            else:
                loop(0, stop, function)

        def owner(q):
            return {"slab": first_slab + q // n_pencil, "pencil": q % n_pencil, "comp": n_comp - 1}

        def owned_by(q):
            return jnp.logical_and(mine == q, me[2] == n_comp - 1)

        def scatter(q):
            return pltpu.make_async_remote_copy(
                src_ref=partial.at[q], dst_ref=RB.at[flat],
                send_sem=send_sem.at[1], recv_sem=recv_sem.at[8],
                device_id=owner(q), device_id_type=MESH,
            )

        def landed(ref, sem):
            pltpu.make_async_copy(ref, ref, sem).wait()

        def gather(q, k):
            return pltpu.make_async_remote_copy(
                src_ref=GB.at[q], dst_ref=GB.at[q],
                send_sem=send_sem.at[2], recv_sem=recv_sem.at[9],
                device_id=device(k), device_id_type=MESH,
            )

        def unless(same, function):
            @pl.when(jnp.logical_not(same))
            def _():
                function()

        mine = (me[0] - first_slab) * n_pencil + me[1]
        owning = jnp.logical_and(
            me[2] == n_comp - 1, jnp.logical_and(mine >= 0, mine < owners)
        )
        with scope("dot"):
            lhs = pooled(rim)
            for cut in range(0, sensors, 256):
                value = acc[:, cut:cut + 256] + jnp.dot(
                    lhs, weight[0, 0:2 * rim, cut:cut + 256], preferred_element_type=F32
                )
                for low in (0, 128):
                    for c in range(3):
                        partial[(cut + low) // piece, c, (cut + low) % piece // 128] = (
                            value[c, low:low + 128]
                        )
        with scope("rssend"):
            for q in range(owners):
                unless(owned_by(q), lambda: scatter(q).start())

        with scope("damage"):
            loop(0, Z, lambda z: damage(1, z))

        @pl.when(owning)
        def _():
            with scope("waitrs"):
                landed(RB.at[0:count - 1], recv_sem.at[8])
            RB[flat] = partial[mine]
            if count <= 16:
                total = RB[0]
                for k in range(1, count):
                    total = total + RB[k]
            else:
                total = lax.fori_loop(1, count, lambda k, t: t + RB[k], RB[0])
            GB[mine] = total
            spread(count, lambda k: unless(flat == k, lambda: gather(mine, k).start()))

        with scope("waitag"):
            @pl.when(owning)
            def _():
                if owners > 1:
                    landed(GB.at[0:owners - 1], recv_sem.at[9])

            @pl.when(jnp.logical_not(owning))
            def _():
                landed(GB.at[0:owners], recv_sem.at[9])

        for q in range(owners):
            for c in range(3):
                for k in range(strips):
                    low = q * piece + 128 * k
                    read_ref[c, low:low + 128] = GB[q, c, k]
        with scope("sends"):
            settle_messages((0, 1), lambda t: SENT[t], send_sem.at[0])

            @pl.when(owning)
            def _():
                if owners > 1:
                    landed(partial.at[0:owners - 1], send_sem.at[1])
                landed(RB.at[0:count - 1], send_sem.at[2])

            @pl.when(jnp.logical_not(owning))
            def _():
                landed(partial.at[0:owners], send_sem.at[1])

    return kernel


def emit(moved_ref, damage_ref, read_ref, moved_hbm, damage_hbm, read_hbm, sem):
    half = damage_ref.shape[0] // 2
    for low in (0, half):
        here = pl.ds(low, half)
        for i in range(moved_ref.shape[0]):
            pltpu.make_async_copy(moved_ref.at[i, here], moved_hbm.at[i, here], sem.at[0]).start()
        pltpu.make_async_copy(damage_ref.at[here], damage_hbm.at[here], sem.at[1]).start()
    last = pltpu.make_async_copy(read_ref, read_hbm, sem.at[2])
    last.start()
    pltpu.make_async_copy(moved_ref, moved_hbm, sem.at[0]).wait()
    pltpu.make_async_copy(damage_ref, damage_hbm, sem.at[1]).wait()
    last.wait()


def solution(mesh):
    sizes = tuple(mesh.shape[a] for a in AXES)
    n_slab = sizes[0]
    count = sizes[0] * sizes[1] * sizes[2]

    def local(u_start, toughness, crack_label, obs_weight, sensor_cell):
        Z, R, C = toughness.shape
        S = sensor_cell.shape[0]
        first_slab = max(n_slab // 2 - 1, 0)
        owners = min(2, n_slab) * sizes[1]
        while S % (owners * 256):
            owners -= 1
        piece = S // owners
        rim, inner = 4 * R, (Z - 4) * R
        most = max(
            Z * R * S * 2 // 4096,
            sum(group_tiles(t, SENT[t], (2, 2, 2), Z, R, C // 128) for t in range(2)),
        )
        any_spec = pl.BlockSpec(memory_space=pltpu.HBM)
        vmem_spec = pl.BlockSpec(memory_space=pltpu.VMEM)
        dma = pltpu.SemaphoreType.DMA
        shapes = (
            jax.ShapeDtypeStruct((3, Z, R, C), F32),
            jax.ShapeDtypeStruct((Z, R, C), F32),
            jax.ShapeDtypeStruct((3, S), F32),
        )
        outs = pl.pallas_call(
            make_kernel(Z, R, C, S, sizes, first_slab, owners),
            out_shape=shapes,
            in_specs=[any_spec] * 5,
            out_specs=[vmem_spec] * 3,
            scratch_shapes=[
                pltpu.VMEM((2, 4, Z + 4, C // 128 + 1, R + 32, 128), F32),
                pltpu.VMEM((2, 2, 4, Z, R, 128), F32),
                pltpu.VMEM((2, 2, 2, 8, 128), F32),
                pltpu.VMEM((2, 2, 2, 8, 128), F32),
                pltpu.VMEM((2, 2, Z + 2, 8, C), F32),
                pltpu.VMEM((2, 2, Z, 8, C), F32),
                pltpu.VMEM((2, 2, 2, 8, C), F32),
                pltpu.VMEM((2, 2, 2, 2, 8, 128), F32),
                pltpu.VMEM((2, 2, 2, 2, 8, 128), F32),
                pltpu.VMEM((Z + 2, 3, R, C), F32),
                pltpu.VMEM((Z, 3, C // 128, R + 32, 128), F32),
                pltpu.VMEM((most, 8, 128), F32),
                pltpu.VMEM((Z, R, C), F32),
                pltpu.VMEM((Z, R, C), jnp.int32),
                pltpu.VMEM((2, 2 * max(rim, inner), S), jnp.bfloat16),
                pltpu.VMEM((1, S), jnp.int32),
                pltpu.VMEM((max(rim, inner), 128), F32),
                pltpu.VMEM((8, S), F32),
                pltpu.VMEM((owners, 3, piece // 128, 128), F32),
                pltpu.VMEM((count, 3, piece // 128, 128), F32),
                pltpu.VMEM((owners, 3, piece // 128, 128), F32),
                dma((6,)),
                dma((3,)),
                dma((11,)),
            ],
            compiler_params=pltpu.CompilerParams(
                collective_id=0, has_side_effects=True, vmem_limit_bytes=40 * 1024 * 1024
            ),
            name="fracture",
        )(
            *[
                pltpu.with_memory_space_constraint(x, pltpu.HBM)
                for x in (
                    u_start, toughness, crack_label, obs_weight.reshape(Z * R, S),
                    sensor_cell.reshape(1, S),
                )
            ],
        )
        return pl.pallas_call(
            emit,
            out_shape=shapes,
            in_specs=[vmem_spec] * 3,
            out_specs=[any_spec] * 3,
            scratch_shapes=[dma((3,))],
            name="emit",
        )(*[pltpu.with_memory_space_constraint(x, pltpu.VMEM) for x in outs])

    return jax.shard_map(
        local,
        mesh=mesh,
        in_specs=(
            P(None, ("groups", "slab"), "pencil", "comp"),
            P(("groups", "slab"), "pencil", "comp"),
            P(("groups", "slab"), "pencil", "comp"),
            P("slab", "pencil", "comp", None),
            P(),
        ),
        out_specs=(
            P(None, ("groups", "slab"), "pencil", "comp"),
            P(("groups", "slab"), "pencil", "comp"),
            P(None, "groups"),
        ),
        check_vma=False,
    )
```

```python
import itertools

import jax
import jax.numpy as jnp
import numpy as np
from jax import lax
from jax.experimental import pallas as pl
from jax.experimental.pallas import tpu as pltpu
from jax.sharding import PartitionSpec as P

RESIDUAL_STIFF = 0.001
TIME_DISP = 0.15
TIME_DAMAGE = 0.08
DAMAGE_LEVEL = 0.45
POINT_GAIN = 8.0
AXES = ("slab", "pencil", "comp")
MESH = pl.DeviceIdType.MESH
F32 = jnp.float32


def third_angle_poly():
    nodes = 0.5 + 0.5 * np.cos(np.pi * (np.arange(200) + 0.5) / 200)
    fit = np.polynomial.chebyshev.Chebyshev.fit(
        nodes, np.cos(np.arccos(nodes) / 3.0), 8, domain=[0.0, 1.0]
    )
    return [float(c) for c in fit.convert(kind=np.polynomial.Polynomial).coef]


POLY = third_angle_poly()

DIRECTIONS = [
    d for d in itertools.product((-1, 0, 1), repeat=3) if 1 <= sum(map(abs, d)) <= 2
]
ALONG_Z = [d for d in DIRECTIONS if d[0] and not d[1] and not d[2]]
ALONG_Y = [d for d in DIRECTIONS if d[1] and not d[0] and not d[2]]
ALONG_X = [d for d in DIRECTIONS if d[2] and not d[0] and not d[1]]
DIAG_ZY = [d for d in DIRECTIONS if d[0] and d[1]]
DIAG_ZX = [d for d in DIRECTIONS if d[0] and d[2]]
DIAG_YX = [d for d in DIRECTIONS if d[1] and d[2]]
KINDS = (
    [("zu", d) for d in ALONG_Z] + [("zy", d) for d in DIAG_ZY] + [("zx", d) for d in DIAG_ZX]
    + [("zd", d) for d in ALONG_Z] + [("zs", d) for d in ALONG_Z]
    + [(k, d) for k in ("y0", "y1", "y2") for d in ALONG_Y]
    + [(k, d) for k in ("yx0", "yx1") for d in DIAG_YX]
    + [(k, d) for k in ("x0", "x1", "x2") for d in ALONG_X]
)
EDGE = ("zu", "zy", "zx")
REST = ("zd", "zs")


def energy_of(g0, g1, g2, a01, a02, a12):
    trace = g0 + g1 + g2
    mean = trace * (1.0 / 3.0)
    d0, d1, d2 = g0 - mean, g1 - mean, g2 - mean
    q01, q02, q12 = a01 * a01, a02 * a02, a12 * a12
    d01 = d0 * d1
    p2 = (d0 * d0 + d1 * d1 + d01) * (1.0 / 3.0) + (q01 + q02 + q12) * (1.0 / 12.0)
    inv = lax.rsqrt(jnp.maximum(p2, 1e-36))
    p = p2 * inv
    det = d01 * d2 + 0.25 * (a01 * a02 * a12 - d0 * q12 - d1 * q02 - d2 * q01)
    half_det = ((det * inv) * inv) * (0.5 * inv)
    r = jnp.minimum(jnp.abs(half_det), 1.0)
    c = jnp.full_like(r, POLY[-1])
    for coefficient in POLY[-2::-1]:
        c = c * r + coefficient
    tc = p * c
    t = jnp.where(half_det < 0.0, -tc, tc)
    s2 = jnp.maximum(1.0 - c * c, 0.0)
    delta = p * (s2 * lax.rsqrt(jnp.maximum(s2, 1e-30))) * float(np.sqrt(3.0))
    f1 = jnp.maximum(mean + 2.0 * t, 0.0)
    f2 = jnp.maximum(mean - t + delta, 0.0)
    f3 = jnp.maximum(mean - t - delta, 0.0)
    ft = jnp.maximum(trace, 0.0)
    return 0.75 * ft * ft + f1 * f1 + f2 * f2 + f3 * f3


def message_tiles(kind, step, Z, R, L):
    if kind in ("zu", "zs"):
        return 3 * L * R // 8
    if kind == "zd":
        return L * R // 8
    if kind == "zx":
        return 1
    if kind == "zy":
        return L
    if kind[:2] == "yx":
        return 1
    planes = 1 if kind[1] != "0" else Z - 2 if step else Z
    return planes * L if kind[0] == "y" else planes * 4 * R // 8


SENT = [
    ("zu", "zx", "zy", "zd", "zs", "y0", "yx0", "x0"),
    ("zu", "zx", "zy", "zd", "zs", "y0", "yx0", "x0", "y1", "y2", "yx1", "x1", "x2"),
]


def group_tiles(step, kinds, met, Z, R, L):
    total = 0
    for kind in kinds:
        number = message_tiles(kind, step, Z, R, L)
        axes = [a for a, name in enumerate("zyx") if name in kind[:2]]
        for a in axes if kind[:2] in ("zx", "zy", "yx") else axes[:1]:
            number *= met[a]
        total += number
    return total


def make_kernel(planes, rows, columns, sensors, sizes, first_slab, owners):
    n_slab, n_pencil, n_comp = sizes
    count = n_slab * n_pencil * n_comp
    Z, R, C = planes, rows, columns
    piece = sensors // owners
    strips = piece // 128
    L = C // 128
    TOP = 16
    END = TOP + R
    body_rows = slice(TOP, END)
    rim = 4 * R
    spans = {
        0: {"0": (0, Z)},
        1: {"0": (1, Z - 1), "1": (0, 1), "2": (Z - 1, Z)},
    }
    groups = {0: [range(Z)], 1: [range(1, Z - 1), [0, Z - 1]]}
    near = n_slab <= 4 and n_pencil <= 2 and n_comp <= 2

    def scope(name):
        return jax.named_scope(name)

    def kernel(u_hbm, tough_hbm, crack_hbm, weight_hbm, cell_hbm,
               moved_ref, damage_ref, read_ref,
               U, XR, XS, XC, YR, YP, YZ, YX, YXR, TZ, TY, W, tough, crack, weight, cell_ref, pooled_t, acc,
               partial, RB, GB,
               in_sem, send_sem, recv_sem):
        me = [lax.axis_index(a) for a in AXES]
        flat = (me[0] * n_pencil + me[1]) * n_comp + me[2]

        def device(index):
            return {
                "slab": index // (n_pencil * n_comp),
                "pencil": (index // n_comp) % n_pencil,
                "comp": index % n_comp,
            }

        def u_load(k, low, high):
            return [
                pltpu.make_async_copy(
                    u_hbm.at[:, low:high, :, 128 * l:128 * l + 128],
                    U.at[0, 0:3, low + 2:high + 2, l, body_rows, :],
                    in_sem.at[4 if k == 2 else 0],
                )
                for l in range(L)
            ]

        edge_loads = u_load(0, 0, 2) + u_load(1, Z - 2, Z)
        inner_loads = u_load(2, 2, Z - 2)
        crack_load = pltpu.make_async_copy(crack_hbm, crack, in_sem.at[1])
        tough_load = pltpu.make_async_copy(tough_hbm, tough, in_sem.at[2])
        cell_load = pltpu.make_async_copy(cell_hbm, cell_ref, in_sem.at[3])
        inner = Z * R - rim
        weight_loads = [
            pltpu.make_async_copy(weight_hbm.at[0:rim // 2], weight.at[0, 0:rim // 2], in_sem.at[5]),
            pltpu.make_async_copy(
                weight_hbm.at[Z * R - rim // 2:Z * R], weight.at[0, rim // 2:rim], in_sem.at[5]),
            pltpu.make_async_copy(
                weight_hbm.at[rim // 2:Z * R - rim // 2], weight.at[1, 0:inner], in_sem.at[5]),
        ]
        for item in edge_loads:
            item.start()

        barrier = pltpu.get_barrier_semaphore()

        def inside(d, sign):
            ok = None
            for m, o, n in zip(me, d, sizes):
                if o:
                    here = m + 1 < n if sign * o > 0 else m >= 1
                    ok = here if ok is None else jnp.logical_and(ok, here)
            return ok

        def feasible(d):
            return all(n > 1 for o, n in zip(d, sizes) if o)

        def neighbour(d):
            return {a: m + o for a, m, o in zip(AXES, me, d)}

        met = 0
        if near:
            for d in DIRECTIONS:
                if feasible(d):
                    @pl.when(inside(d, 1))
                    def _():
                        pl.semaphore_signal(
                            barrier, inc=1, device_id=neighbour(d), device_id_type=MESH
                        )

                    met = met + inside(d, 1).astype(jnp.int32)
        else:
            def greet(k, carry):
                pl.semaphore_signal(
                    barrier, inc=1, device_id=device((flat + k) % count), device_id_type=MESH
                )
                return carry

            lax.fori_loop(1, count, greet, 0)
            met = count - 1

        for item in [crack_load, *inner_loads, cell_load]:
            item.start()

        def clear(d, write):
            if feasible(d):
                @pl.when(jnp.logical_not(inside(d, 1)))
                def _():
                    write()
            else:
                write()

        def clear_z(up):
            def write():
                for step in range(2):
                    for z in ((Z + 2, Z + 3) if up else (0, 1)):
                        U[step, :, z, 0:L, body_rows] = jnp.zeros((4, L, R, 128), F32)
                XC[:, up] = jnp.zeros((2, 2, 8, 128), F32)
                for step in range(2):
                    for side in range(2):
                        YR[step, side, (Z + 1) * up] = jnp.zeros((8, C), F32)
            return write

        def clear_x(right):
            def write():
                def one(k, carry):
                    XR[k // (4 * Z), right, (k // Z) % 4, k % Z] = jnp.zeros((R, 128), F32)
                    return carry

                lax.fori_loop(0, 8 * Z, one, 0)
                XC[:, :, right] = jnp.zeros((2, 2, 8, 128), F32)
                YXR[:, :, right] = jnp.zeros((2, 2, 2, 8, 128), F32)
            return write

        def clear_y(up):
            def write():
                YR[:, up] = jnp.zeros((2, Z + 2, 8, C), F32)
                YXR[:, up] = jnp.zeros((2, 2, 2, 8, 128), F32)
            return write

        core_rows = range(TOP, END, 8)
        row8t = lax.broadcasted_iota(jnp.int32, (8, 128), 0)
        lane8 = lax.broadcasted_iota(jnp.int32, (8, 128), 1)
        lane_r = lax.broadcasted_iota(jnp.int32, (R, 128), 1)

        def roll(value, shift, axis):
            shift = shift % value.shape[axis]
            return pltpu.roll(value, shift, axis) if shift else value

        def loop(start, stop, function):
            def one(z, carry):
                function(z)
                return carry

            lax.fori_loop(start, stop, one, 0)

        def slot(step, kind):
            if step == 0:
                return 11 if kind == "zu" else 0 if kind in EDGE else 1 if kind in REST else 2 if kind[0] == "x" else 3
            if kind[0] == "z":
                return 4
            if kind[-1] == "0":
                return 5 if kind[0] == "x" else 6
            return 10 if kind[0] == "x" else 7

        def message(step, kind, d):
            dz, dy, dx = d
            sz, sy, sx = (dz + 1) // 2, (dy + 1) // 2, (dx + 1) // 2
            tile = L - 1 if dx > 0 else 0
            edge = Z - 1 if dz > 0 else 0
            halo = 0 if dz > 0 else Z + 1
            if kind == "zu":
                pair = (
                    U.at[step, 0:3, edge + 2, 0:L, body_rows], U.at[step, 0:3, halo + 1, 0:L, body_rows]
                )
            elif kind == "zs":
                pair = (
                    U.at[step, 0:3, Z if dz > 0 else 3, 0:L, body_rows],
                    U.at[step, 0:3, 0 if dz > 0 else Z + 3, 0:L, body_rows],
                )
            elif kind == "zd":
                pair = (U.at[step, 3, edge + 2, 0:L, body_rows], U.at[step, 3, halo + 1, 0:L, body_rows])
            elif kind == "zy":
                pair = (YZ.at[step, sy, sz], YR.at[step, 1 - sy, halo])
            elif kind == "zx":
                pair = (XS.at[step, sz, sx], XC.at[step, 1 - sz, 1 - sx])
            elif kind[:2] == "yx":
                part = int(kind[2])
                pair = (YX.at[step, sy, sx, part], YXR.at[step, 1 - sy, 1 - sx, part])
            else:
                low, high = spans[step][kind[1]]
                if kind[0] == "y":
                    pair = (YP.at[step, sy, low:high], YR.at[step, 1 - sy, low + 1:high + 1])
                else:
                    pair = (
                        U.at[step, :, low + 2:high + 2, tile, body_rows],
                        XR.at[step, 1 - sx, :, low:high],
                    )
            return pltpu.make_async_remote_copy(
                src_ref=pair[0],
                dst_ref=pair[1],
                send_sem=send_sem.at[0],
                recv_sem=recv_sem.at[slot(step, kind)],
                device_id=neighbour(d),
                device_id_type=MESH,
            )

        def each(step, kinds, sign, action):
            for name in kinds:
                for kind, d in KINDS:
                    if kind == name and feasible(d):
                        @pl.when(inside(d, sign))
                        def _():
                            action(message(step, kind, d))

        def settle(tiles, sem):
            if tiles:
                pltpu.make_async_copy(W.at[0:tiles], W.at[0:tiles], sem).wait()

        def settle_messages(steps, kinds, sem):
            for number in itertools.product(*[
                (0,) if n == 1 else (1,) if n == 2 else (1, 2) for n in sizes
            ]):
                here = None
                for m, n, k in zip(me, sizes, number):
                    if n > 2:
                        both = jnp.logical_and(m > 0, m < n - 1)
                        ok = both if k == 2 else jnp.logical_not(both)
                        here = ok if here is None else jnp.logical_and(here, ok)
                tiles = sum(group_tiles(t, kinds(t), number, Z, R, L) for t in steps)

                def wait():
                    settle(tiles, sem)

                if here is None:
                    wait()
                else:
                    pl.when(here)(wait)

        def send(step, *kinds):
            each(step, kinds, 1, lambda copy: copy.start())

        def receive(step, *kinds):
            settle_messages((step,), lambda _: kinds, recv_sem.at[slot(step, kinds[0])])

        def pack_plane(step, z, save):
            for side, firsts in (
                (0, [TOP - 2 * f for f in range(4)]),
                (1, [END - 2 - 2 * f for f in range(3)] + [END - 7]),
            ):
                for l in range(L):
                    rows = [U[step, f, z + 2, l, at:at + 8, :] for f, at in enumerate(firsts)]
                    save(side, l, jnp.where(
                        row8t < 2, rows[0],
                        jnp.where(row8t < 4, rows[1], jnp.where(row8t < 6, rows[2], rows[3])),
                    ))

        def pack_y(step, part):
            for z in groups[step][part]:
                def save(side, l, value):
                    YP[step, side, z, :, 128 * l:128 * l + 128] = value

                pack_plane(step, z, save)
            for side in range(2):
                for sx in range(2):
                    tile = jnp.zeros((8, 128), F32)
                    for z in groups[step][part]:
                        value = YP[step, side, z, :, (C - 128) * sx:(C - 128) * sx + 128]
                        tile = jnp.where(lane8 == z, roll(value, z + sx, 1), tile)
                    YX[step, side, sx, part] = tile

        def pack_corners(step):
            for sz, z in ((0, 0), (1, Z - 1)):
                for sx in range(2):
                    tile = jnp.zeros((8, 128), F32)
                    for k, row in enumerate(core_rows):
                        for f in range(3):
                            value = U[step, f, z + 2, (L - 1) * sx, row:row + 8, :]
                            lane = 3 * k + f
                            tile = jnp.where(lane8 == lane, roll(value, lane + sx, 1), tile)
                    XS[step, sz, sx] = tile

                def save(side, l, value):
                    YZ[step, side, sz, :, 128 * l:128 * l + 128] = value

                pack_plane(step, z, save)

        def unpack_x(step, z):
            for f in range(4):
                U[step, f, z + 2, L, body_rows, :] = jnp.where(
                    lane_r < 64, XR[step, 1, f, z], XR[step, 0, f, z]
                )

        def unpack_zx(step):
            for sz, z in ((0, -1), (1, Z)):
                right, left = XC[step, sz, 1], XC[step, sz, 0]
                for k, row in enumerate(core_rows):
                    for f in range(3):
                        lane = 3 * k + f
                        U[step, f, z + 2, L, row:row + 8, :] = jnp.where(
                            lane8 < 64, roll(right, -lane, 1), roll(left, 127 - lane, 1)
                        )

        def put_rows(step, z, l, low, high, fields):
            for f in range(fields):
                if f < 3:
                    U[step, f, z + 2, l, TOP - 2:TOP, :] = low[2 * f:2 * f + 2]
                    U[step, f, z + 2, l, END:END + 2, :] = high[2 * f:2 * f + 2]
                else:
                    U[step, f, z + 2, l, TOP - 1:TOP, :] = low[6:7]
                    U[step, f, z + 2, l, END:END + 1, :] = high[6:7]

        def unpack_y(step, z, fields):
            for l in range(L):
                low, high = [YR[step, side, z + 1, :, 128 * l:128 * l + 128] for side in range(2)]
                put_rows(step, z, l, low, high, fields)

        def unpack_yx(step, part):
            for z in groups[step][part]:
                low, high = [
                    jnp.where(
                        lane8 < 64, roll(YXR[step, sy, 1, part], -z, 1),
                        roll(YXR[step, sy, 0, part], 127 - z, 1),
                    )
                    for sy in range(2)
                ]
                put_rows(step, z, L, low, high, 3)

        def take(step, f, z, row, tiles):
            parts = [U[step, f, z, l, row:row + 8, :] for l in range(tiles)]
            return jnp.concatenate(parts, axis=1)

        def slope_z(step, f, z, row, tiles):
            return take(step, f, z + 3, row, tiles) - take(step, f, z + 1, row, tiles)

        def slope_y(step, f, z, row, tiles):
            return take(step, f, z + 2, row + 1, tiles) - take(step, f, z + 2, row - 1, tiles)

        def beside(value, tiles):
            parts = [value[:, 128 * l:128 * l + 128] for l in range(L + 1)]
            after, before = [], []
            for l in range(tiles):
                after.append(roll(jnp.where(lane8 == 0, parts[(l + 1) % (L + 1)], parts[l]), -1, 1))
                before.append(roll(jnp.where(lane8 == 127, parts[l - 1], parts[l]), 1, 1))
            return jnp.concatenate(after, axis=1), jnp.concatenate(before, axis=1)

        def along_x(value, tiles):
            after, before = beside(value, tiles)
            return after - before

        def slope_x(step, f, z, row):
            return along_x(take(step, f, z + 2, row, L + 1), L)

        def gain(step, z, row, tiles):
            keep = 1.0 - take(step, 3, z + 2, row, tiles)
            return (0.5 * TIME_DISP) * (keep * keep + RESIDUAL_STIFF)

        def store(step, f, z, row, value):
            if step == 0:
                for l in range(L):
                    U[1, f, z + 2, l, row:row + 8, :] = value[:, 128 * l:128 * l + 128]
            elif f < 3:
                moved_ref[f, z, row - TOP:row - TOP + 8, :] = value
            else:
                damage_ref[z, row - TOP:row - TOP + 8, :] = value

        def ends(step, z):
            for row in core_rows:
                gz = [slope_z(step, f, z, row, L) for f in range(3)]
                gy0, gy1 = slope_y(step, 0, z, row, L), slope_y(step, 1, z, row, L)
                gx0, gx2 = slope_x(step, 0, z, row), slope_x(step, 2, z, row)
                g = gain(step, z, row, L)
                h = 0.5 * g
                at = slice(row - TOP, row - TOP + 8)
                TZ[z + 1, 0, at] = g * (gz[0] + 0.75 * (gz[0] + gy1 + gx2))
                TZ[z + 1, 1, at] = h * (gz[1] + gy0)
                TZ[z + 1, 2, at] = h * (gz[2] + gx0)

        def hurt(step, z, row, gz0, gy1, gx2, a01, a02, a12):
            energy = energy_of(gz0, gy1, gx2, a01, a02, a12)
            dx = take(step, 3, z + 2, row, L + 1)
            dc = dx[:, 0:C]
            after, before = beside(dx, L)
            lap = (
                take(step, 3, z + 3, row, L) + take(step, 3, z + 1, row, L)
                + take(step, 3, z + 2, row + 1, L) + take(step, 3, z + 2, row - 1, L)
                + (after + before)
                - 7.0 * dc
            )
            store(step, 3, z, row, dc + TIME_DAMAGE * (
                0.5 * (1.0 - dc) * energy + tough[z, row - TOP:row - TOP + 8, :] * lap
            ))

        def damage(step, z):
            for row in core_rows:
                gz = [slope_z(step, f, z, row, L) for f in range(3)]
                gy = [slope_y(step, f, z, row, L) for f in range(3)]
                gx = [slope_x(step, f, z, row) for f in range(3)]
                hurt(
                    step, z, row, gz[0], gy[1], gx[2],
                    gz[1] + gy[0], gz[2] + gx[0], gy[2] + gx[1],
                )

        def put_y(z, row, values):
            for i in range(3):
                for l in range(L):
                    TY[z, i, l, row:row + 8, :] = values[i][:, 128 * l:128 * l + 128]

        def outer_rows(step, z, flat=False):
            for row in (TOP - 8, END):
                gy = [slope_y(step, f, z, row, L) for f in range(3)]
                gx1, gx2 = [slope_x(step, f, z, row) for f in (1, 2)]
                g = gain(step, z, row, L)
                h = 0.5 * g
                a01, trace = gy[0], gy[1] + gx2
                if not flat:
                    a01 = a01 + slope_z(step, 1, z, row, L)
                    trace = trace + slope_z(step, 0, z, row, L)
                put_y(z, row, [h * a01, g * (gy[1] + 0.75 * trace), h * (gy[2] + gx1)])

        def close(step, z, row, waiting):
            for i in range(3):
                change = jnp.concatenate(
                    [TY[z, i, l, row + 1:row + 9, :] - TY[z, i, l, row - 1:row + 7, :] for l in range(L)],
                    axis=1,
                )
                store(step, i, z, row, waiting[i] + change)

        def held(step, i, z, row):
            if step:
                return moved_ref[i, z, row - TOP:row - TOP + 8, :]
            return take(1, i, z + 2, row, L)

        def strip(step, z, row, with_damage, flat=False):
            wide = L + 1
            now = [take(step, f, z + 2, row, wide) for f in range(3)]
            gy = [slope_y(step, f, z, row, wide) for f in range(3)]
            gx = [along_x(v, wide) for v in now]
            g = gain(step, z, row, wide)
            h = 0.5 * g
            trace = gy[1] + gx[2]
            a01 = gy[0][:, 0:C]
            a02 = gx[0]
            if not flat:
                gz = [slope_z(step, f, z, row, wide) for f in range(3)]
                trace = trace + gz[0]
                a01 = a01 + gz[1][:, 0:C]
                a02 = a02 + gz[2]
            lam = 0.75 * trace
            a12 = gy[2] + gx[1]
            t01, t02, t12 = h[:, 0:C] * a01, h * a02, h * a12
            put_y(z, row, [t01, (g * (gy[1] + lam))[:, 0:C], t12[:, 0:C]])
            at = slice(row - TOP, row - TOP + 8)
            TZ[z + 1, 0, at] = (g * (lam if flat else gz[0] + lam))[:, 0:C]
            TZ[z + 1, 1, at] = t01
            TZ[z + 1, 2, at] = t02[:, 0:C]
            if with_damage:
                hurt(
                    step, z, row, gz[0][:, 0:C], gy[1][:, 0:C], gx[2][:, 0:C],
                    a01, a02[:, 0:C], a12[:, 0:C],
                )
            return [
                now[i][:, 0:C] + along_x(t, L) for i, t in enumerate((t02, t12, g * (gx[2] + lam)))
            ]

        def force_mid(step, z, with_damage, flat=False):
            for row in core_rows[1:-1]:
                for i, value in enumerate(strip(step, z, row, with_damage, flat)):
                    store(step, i, z, row, value)

        def force_rim(step, z, with_damage, flat=False):
            outer_rows(step, z, flat)
            first = strip(step, z, core_rows[0], with_damage, flat)
            last = strip(step, z, core_rows[-1], with_damage, flat)
            close(step, z, core_rows[0], first)
            for row in core_rows[1:-1]:
                close(step, z, row, [held(step, i, z, row) for i in range(3)])
            close(step, z, core_rows[-1], last)

        def force(step, z):
            outer_rows(step, z)
            waiting = None
            for row in core_rows:
                ready = strip(step, z, row, False)
                if waiting is not None:
                    close(step, z, row - 8, waiting)
                waiting = ready
            close(step, z, END - 8, waiting)

        def add_z(z):
            def put(row, first, second):
                for l in range(L):
                    lanes = slice(128 * l, 128 * l + 128)
                    TY[z, 0, l, row:row + 8, :] = first[:, lanes]
                    TY[z, 1, l, row:row + 8, :] = second[:, lanes]

            def close_two(row, waiting):
                at = slice(row - TOP, row - TOP + 8)
                for i in range(3):
                    value = moved_ref[i, z, at, :]
                    if i != 1:
                        value = value + waiting[i // 2]
                    if i < 2:
                        value = value + jnp.concatenate(
                            [
                                TY[z, i, l, row + 1:row + 9, :] - TY[z, i, l, row - 1:row + 7, :]
                                for l in range(L)
                            ],
                            axis=1,
                        )
                    moved_ref[i, z, at, :] = value

            for row in (TOP - 8, END):
                g = gain(1, z, row, L)
                put(
                    row, (0.5 * g) * slope_z(1, 1, z, row, L),
                    (0.75 * g) * slope_z(1, 0, z, row, L),
                )
            waiting = None
            for row in core_rows:
                at = slice(row - TOP, row - TOP + 8)
                g = gain(1, z, row, L + 1)
                h = 0.5 * g
                p = g * slope_z(1, 0, z, row, L + 1)
                q1 = h[:, 0:C] * slope_z(1, 1, z, row, L)
                q2 = h * slope_z(1, 2, z, row, L + 1)
                lam = 0.75 * p
                put(row, q1, lam[:, 0:C])
                TZ[z + 1, 0, at] = TZ[z + 1, 0, at] + (p + lam)[:, 0:C]
                TZ[z + 1, 1, at] = TZ[z + 1, 1, at] + q1
                TZ[z + 1, 2, at] = TZ[z + 1, 2, at] + q2[:, 0:C]
                ready = [along_x(q2, L), along_x(lam, L)]
                if waiting is not None:
                    close_two(row - 8, waiting)
                waiting = ready
            close_two(END - 8, waiting)

        def finish(step, z):
            for i in range(3):
                for l in range(L):
                    lanes = slice(128 * l, 128 * l + 128)
                    U[1, i, z + 2, l, body_rows, :] = U[1, i, z + 2, l, body_rows, :] + (
                        TZ[z + 2, i, :, lanes] - TZ[z, i, :, lanes]
                    )

        def finish_pool(z, row):
            means = []
            for i in range(3):
                value = moved_ref[i, z] + (TZ[z + 2, i] - TZ[z, i])
                moved_ref[i, z] = value
                folded = value[:, 0:128]
                for cut in range(128, C, 128):
                    folded = folded + value[:, cut:cut + 128]
                means.append(jnp.sum(folded, axis=1, keepdims=True) * (1.0 / C))
            pooled_t[row:row + R, :] = jnp.where(
                lane_r == 0, means[0], jnp.where(lane_r == 1, means[1], means[2])
            )

        def pooled(rows_here):
            value = pooled_t[0:rows_here, :].T[0:8].astype(jnp.bfloat16)
            return jnp.concatenate([value, value], axis=1)

        settle(2 * 3 * 2 * L * R // 8, in_sem.at[0])
        with scope("barrier"):
            pl.semaphore_wait(barrier, met)
        send(0, "zu")
        crack_load.wait()

        def label(z, carry):
            for l in range(L):
                U[0, 3, z + 2, l, body_rows, :] = DAMAGE_LEVEL * crack[
                    z, :, 128 * l:128 * l + 128
                ].astype(F32)
            return carry

        lax.fori_loop(0, Z, label, 0)
        settle(3 * (Z - 4) * L * R // 8, in_sem.at[4])
        with scope("pack"):
            pack_y(0, 0)
            send(0, "y0", "yx0", "x0")
            pack_corners(0)
            send(0, "zx", "zy")
            for item in [tough_load, *weight_loads]:
                item.start()
        for side, sign in ((0, -1), (1, 1)):
            clear((sign, 0, 0), clear_z(side))
            clear((0, sign, 0), clear_y(side))
            clear((0, 0, sign), clear_x(side))

        cell_load.wait()
        base = me[0] * Z * (R * n_pencil) + me[1] * R
        row_id = lax.broadcasted_iota(jnp.int32, (R, 512), 0) * n_comp

        def choose(part, z, row):
            start = (base + z * (R * n_pencil)) * n_comp + me[2]
            for s in range(0, sensors, 512):
                hit = row_id == cell_ref[:, s:s + 512] - start
                weight[part, row:row + R, s:s + 512] = jnp.where(hit, POINT_GAIN, 0.0).astype(
                    jnp.bfloat16
                )

        with scope("choose"):
            for k, z in enumerate((0, 1, Z - 2, Z - 1)):
                choose(0, z, rim + k * R)
            for z in range(2, Z - 2):
                choose(1, z, inner + (z - 2) * R)
            tough_load.wait()
        send(0, "zd", "zs")
        with scope("waitx"):
            receive(0, "x0")
        with scope("unpx"):
            loop(0, Z, lambda z: unpack_x(0, z))
        with scope("mid"):
            loop(1, Z - 1, lambda z: force_mid(0, z, True))
        with scope("waity"):
            receive(0, "y0", "yx0")
        with scope("unpy"):
            loop(0, Z, lambda z: unpack_y(0, z, 4))
            unpack_yx(0, 0)
        with scope("body"):
            loop(0, 2, lambda k: force_rim(0, 2 + k * (Z - 5), True))
            loop(0, 2, lambda k: force_rim(0, 1 + k * (Z - 3), True))
        with scope("waitza"):
            receive(0, "zu")
        with scope("edge"):
            loop(0, 2, lambda k: ends(0, k * (Z - 1)))
            loop(0, 2, lambda k: finish(0, 1 + k * (Z - 3)))
        send(1, "zs")
        with scope("body2"):
            loop(3, Z - 3, lambda z: force_rim(0, z, True))
            loop(2, Z - 2, lambda z: finish(0, z))
            pack_y(1, 0)
            send(1, "y0", "yx0", "x0")
            receive(0, "zx", "zy")
            unpack_zx(0)
            for z in (-1, Z):
                unpack_y(0, z, 3)
            loop(0, 2, lambda k: force(0, k * (Z - 1)))
        with scope("waitzb"):
            receive(0, *REST)
        with scope("ends"):
            loop(0, 2, lambda k: ends(0, k * (Z + 1) - 1))
            loop(0, 2, lambda k: finish(0, k * (Z - 1)))
        pack_corners(1)
        send(1, "zu", "zx", "zy")
        with scope("damage"):
            loop(0, 2, lambda k: damage(0, k * (Z - 1)))
        send(1, "zd")
        with scope("pack2"):
            pack_y(1, 1)
            send(1, "y1", "y2", "yx1", "x1", "x2")

        with scope("waitx"):
            receive(1, "x0")
            loop(1, Z - 1, lambda z: unpack_x(1, z))
        with scope("mid"):
            loop(2, Z - 2, lambda z: force_mid(1, z, False))
        with scope("waitxe"):
            receive(1, "x1", "x2")
        with scope("mide"):
            for z in (0, Z - 1):
                unpack_x(1, z)
            loop(0, 2, lambda k: force_mid(1, 1 + k * (Z - 3), False))
            loop(0, 2, lambda k: force_mid(1, k * (Z - 1), False, True))
        with scope("waity"):
            receive(1, "y0", "yx0")
            loop(1, Z - 1, lambda z: unpack_y(1, z, 4))
            unpack_yx(1, 0)
        with scope("rim"):
            loop(2, Z - 2, lambda z: force_rim(1, z, False))
        with scope("waitye"):
            receive(1, "y1", "y2", "yx1")
        with scope("rime"):
            for z in (0, Z - 1):
                unpack_y(1, z, 4)
            unpack_yx(1, 1)
            loop(0, 2, lambda k: force_rim(1, 1 + k * (Z - 3), False))
        with scope("pooli"):
            for z in range(2, Z - 2):
                finish_pool(z, (z - 2) * R)
        with scope("doti"):
            settle(Z * R * sensors * 2 // 4096, in_sem.at[5])
            lhs = pooled(inner)
            for cut in range(0, sensors, 256):
                acc[:, cut:cut + 256] = jnp.dot(
                    lhs, weight[1, 0:2 * inner, cut:cut + 256], preferred_element_type=F32
                )
        with scope("flat"):
            loop(0, 2, lambda k: force_rim(1, k * (Z - 1), False, True))
        with scope("waitz"):
            receive(1, *REST, *EDGE)
        with scope("edge"):
            unpack_zx(1)
            for z in (-1, Z):
                unpack_y(1, z, 3)
            for k in range(2):
                ends(1, k * (Z + 1) - 1)
                add_z(k * (Z - 1))
        with scope("poole"):
            for k, z in enumerate((0, 1, Z - 2, Z - 1)):
                finish_pool(z, k * R)

        def spread(stop, function):
            if stop <= 16:
                for k in range(stop):
                    function(k)
            else:
                loop(0, stop, function)

        def owner(q):
            return {"slab": first_slab + q // n_pencil, "pencil": q % n_pencil, "comp": n_comp - 1}

        def owned_by(q):
            return jnp.logical_and(mine == q, me[2] == n_comp - 1)

        def scatter(q):
            return pltpu.make_async_remote_copy(
                src_ref=partial.at[q], dst_ref=RB.at[flat],
                send_sem=send_sem.at[1], recv_sem=recv_sem.at[8],
                device_id=owner(q), device_id_type=MESH,
            )

        def landed(ref, sem):
            pltpu.make_async_copy(ref, ref, sem).wait()

        def gather(q, k):
            return pltpu.make_async_remote_copy(
                src_ref=GB.at[q], dst_ref=GB.at[q],
                send_sem=send_sem.at[2], recv_sem=recv_sem.at[9],
                device_id=device(k), device_id_type=MESH,
            )

        def unless(same, function):
            @pl.when(jnp.logical_not(same))
            def _():
                function()

        mine = (me[0] - first_slab) * n_pencil + me[1]
        owning = jnp.logical_and(
            me[2] == n_comp - 1, jnp.logical_and(mine >= 0, mine < owners)
        )
        with scope("dot"):
            lhs = pooled(rim)
            for cut in range(0, sensors, 256):
                value = acc[:, cut:cut + 256] + jnp.dot(
                    lhs, weight[0, 0:2 * rim, cut:cut + 256], preferred_element_type=F32
                )
                for low in (0, 128):
                    for c in range(3):
                        partial[(cut + low) // piece, c, (cut + low) % piece // 128] = (
                            value[c, low:low + 128]
                        )
        with scope("rssend"):
            for q in range(owners):
                unless(owned_by(q), lambda: scatter(q).start())

        with scope("damage"):
            loop(0, Z, lambda z: damage(1, z))

        @pl.when(owning)
        def _():
            with scope("waitrs"):
                landed(RB.at[0:count - 1], recv_sem.at[8])
            RB[flat] = partial[mine]
            if count <= 16:
                total = RB[0]
                for k in range(1, count):
                    total = total + RB[k]
            else:
                total = lax.fori_loop(1, count, lambda k, t: t + RB[k], RB[0])
            GB[mine] = total
            spread(count, lambda k: unless(flat == k, lambda: gather(mine, k).start()))

        with scope("waitag"):
            @pl.when(owning)
            def _():
                if owners > 1:
                    landed(GB.at[0:owners - 1], recv_sem.at[9])

            @pl.when(jnp.logical_not(owning))
            def _():
                landed(GB.at[0:owners], recv_sem.at[9])

        for q in range(owners):
            for c in range(3):
                for k in range(strips):
                    low = q * piece + 128 * k
                    read_ref[c, low:low + 128] = GB[q, c, k]
        with scope("sends"):
            settle_messages((0, 1), lambda t: SENT[t], send_sem.at[0])

            @pl.when(owning)
            def _():
                if owners > 1:
                    landed(partial.at[0:owners - 1], send_sem.at[1])
                landed(RB.at[0:count - 1], send_sem.at[2])

            @pl.when(jnp.logical_not(owning))
            def _():
                landed(partial.at[0:owners], send_sem.at[1])

    return kernel


def emit(moved_ref, damage_ref, read_ref, moved_hbm, damage_hbm, read_hbm, sem):
    half = damage_ref.shape[0] // 2
    for low in (0, half):
        here = pl.ds(low, half)
        for i in range(moved_ref.shape[0]):
            pltpu.make_async_copy(moved_ref.at[i, here], moved_hbm.at[i, here], sem.at[0]).start()
        pltpu.make_async_copy(damage_ref.at[here], damage_hbm.at[here], sem.at[1]).start()
    last = pltpu.make_async_copy(read_ref, read_hbm, sem.at[2])
    last.start()
    pltpu.make_async_copy(moved_ref, moved_hbm, sem.at[0]).wait()
    pltpu.make_async_copy(damage_ref, damage_hbm, sem.at[1]).wait()
    last.wait()


def solution(mesh):
    sizes = tuple(mesh.shape[a] for a in AXES)
    n_slab = sizes[0]
    count = sizes[0] * sizes[1] * sizes[2]

    def local(u_start, toughness, crack_label, obs_weight, sensor_cell):
        Z, R, C = toughness.shape
        S = sensor_cell.shape[0]
        first_slab = max(n_slab // 2 - 1, 0)
        owners = min(2, n_slab) * sizes[1]
        while S % (owners * 256):
            owners -= 1
        piece = S // owners
        rim, inner = 4 * R, (Z - 4) * R
        most = max(
            Z * R * S * 2 // 4096,
            sum(group_tiles(t, SENT[t], (2, 2, 2), Z, R, C // 128) for t in range(2)),
        )
        any_spec = pl.BlockSpec(memory_space=pltpu.HBM)
        vmem_spec = pl.BlockSpec(memory_space=pltpu.VMEM)
        dma = pltpu.SemaphoreType.DMA
        shapes = (
            jax.ShapeDtypeStruct((3, Z, R, C), F32),
            jax.ShapeDtypeStruct((Z, R, C), F32),
            jax.ShapeDtypeStruct((3, S), F32),
        )
        outs = pl.pallas_call(
            make_kernel(Z, R, C, S, sizes, first_slab, owners),
            out_shape=shapes,
            in_specs=[any_spec] * 5,
            out_specs=[vmem_spec] * 3,
            scratch_shapes=[
                pltpu.VMEM((2, 4, Z + 4, C // 128 + 1, R + 32, 128), F32),
                pltpu.VMEM((2, 2, 4, Z, R, 128), F32),
                pltpu.VMEM((2, 2, 2, 8, 128), F32),
                pltpu.VMEM((2, 2, 2, 8, 128), F32),
                pltpu.VMEM((2, 2, Z + 2, 8, C), F32),
                pltpu.VMEM((2, 2, Z, 8, C), F32),
                pltpu.VMEM((2, 2, 2, 8, C), F32),
                pltpu.VMEM((2, 2, 2, 2, 8, 128), F32),
                pltpu.VMEM((2, 2, 2, 2, 8, 128), F32),
                pltpu.VMEM((Z + 2, 3, R, C), F32),
                pltpu.VMEM((Z, 3, C // 128, R + 32, 128), F32),
                pltpu.VMEM((most, 8, 128), F32),
                pltpu.VMEM((Z, R, C), F32),
                pltpu.VMEM((Z, R, C), jnp.int32),
                pltpu.VMEM((2, 2 * max(rim, inner), S), jnp.bfloat16),
                pltpu.VMEM((1, S), jnp.int32),
                pltpu.VMEM((max(rim, inner), 128), F32),
                pltpu.VMEM((8, S), F32),
                pltpu.VMEM((owners, 3, piece // 128, 128), F32),
                pltpu.VMEM((count, 3, piece // 128, 128), F32),
                pltpu.VMEM((owners, 3, piece // 128, 128), F32),
                dma((6,)),
                dma((3,)),
                dma((12,)),
            ],
            compiler_params=pltpu.CompilerParams(
                collective_id=0, has_side_effects=True, vmem_limit_bytes=40 * 1024 * 1024
            ),
            name="fracture",
        )(
            *[
                pltpu.with_memory_space_constraint(x, pltpu.HBM)
                for x in (
                    u_start, toughness, crack_label, obs_weight.reshape(Z * R, S),
                    sensor_cell.reshape(1, S),
                )
            ],
        )
        return pl.pallas_call(
            emit,
            out_shape=shapes,
            in_specs=[vmem_spec] * 3,
            out_specs=[any_spec] * 3,
            scratch_shapes=[dma((3,))],
            name="emit",
        )(*[pltpu.with_memory_space_constraint(x, pltpu.VMEM) for x in outs])

    return jax.shard_map(
        local,
        mesh=mesh,
        in_specs=(
            P(None, ("groups", "slab"), "pencil", "comp"),
            P(("groups", "slab"), "pencil", "comp"),
            P(("groups", "slab"), "pencil", "comp"),
            P("slab", "pencil", "comp", None),
            P(),
        ),
        out_specs=(
            P(None, ("groups", "slab"), "pencil", "comp"),
            P(("groups", "slab"), "pencil", "comp"),
            P(None, "groups"),
        ),
        check_vma=False,
    )
```
